256 devices in a mesh: sec: 8 (over x, core), op: 32 (over y, z).
Axes of the slice: x: 4, y: 4, z: 8, core: 2. Of those that a mesh axis runs over, the one named last changes fastest.
Arguments:
- wavefunction: bfloat16 [8, 768, 768], P('sec', 'op'), may hold values from -6 to 6
- left_ops: bfloat16 [8, 96, 768, 768], P('sec', 'op'), may hold values from -0.0234375 to 0.0234375
- right_ops: bfloat16 [8, 96, 768, 768], P('sec', 'op'), may hold values from -0.21875 to 0.21875
- diagonal: float32 [8, 768, 768], P('sec', 'op'), may hold values from 0.15 to 10.2
- sector_sizes: int32 [8], P('sec'), may hold values from 192 to 768
- partner: int32 [8], replicated, may hold values from 0 to 7, as said below
Outputs:
- updated: float32 [8, 768, 768], P('sec', 'op')
- residual: float32 [8, 768, 768], P('sec', 'op')
The draws below stay inside these ranges and needn't reach their ends.
Inputs may be any that keep to these rules, and one draw needn't show every extreme that they name: `partner`: each sector is named exactly once.
All inputs are finite; a program needn't handle non-finite values.
Results may differ from the reference program's by a relative error of at most 0.0017.
Values may be sent and summed in bfloat16 or wider, within the bound.
No kernel may reach another device: no remote copies, remote signals or barrier semaphores. Data moves between devices by JAX's collectives and lax.ppermute only.
A program may use at most 64 MiB of HBM per device.

```python
import jax
import jax.numpy as jnp
from jax import lax

B = 768
SECTORS = 8
TERMS = 96


def draw_diagonal(key, part):
    noise_key = jax.random.fold_in(key, 7)
    sector_pos = jnp.arange(SECTORS, dtype=jnp.float32) / float(max(SECTORS - 1, 1))
    row_pos = jnp.arange(B, dtype=jnp.float32) / float(max(B - 1, 1))
    level = 0.5 + 1.5 * sector_pos
    rising = 1.0 + 2.0 * row_pos
    noise = jax.random.uniform(noise_key, (SECTORS, B, B), jnp.float32, 0.6, 1.4)
    return level[:, None, None] * rising[None, :, None] * noise


def draw_partner(key, part):
    order_key = jax.random.fold_in(key, 11)
    shuffled = jax.random.permutation(order_key, SECTORS).astype(jnp.int32)
    middle = SECTORS // 2
    first_value = shuffled[0]
    places = jnp.arange(SECTORS, dtype=jnp.int32)
    swapped = jnp.where(shuffled == middle, first_value, shuffled)
    return jnp.where(places == 0, jnp.int32(middle), swapped).astype(jnp.int32)


def touch_ends(drawn, stream_key, smallest, largest):
    shape = drawn.shape
    place = [jax.random.randint(jax.random.fold_in(stream_key, axis), (), 0, shape[axis]) for axis in range(len(shape))]
    drawn = drawn.at[tuple(place)].set(smallest)
    longest = shape.index(max(shape))
    place[longest] = (place[longest] + 1) % shape[longest]
    return drawn.at[tuple(place)].set(largest)


def level_of(key, dims, shards, low, top_value):
    def one(position, shards_of):
        draws = jax.random.uniform(jax.random.fold_in(jax.random.fold_in(key, 6), position), (shards_of,), jnp.float32, low / len(shards), top_value / len(shards))
        return jnp.repeat(jnp.exp(draws), dims[position] // shards_of).reshape((-1,) + (1,) * (len(dims) - position - 1))

    level = one(*shards[0])
    for cut in shards[1:]:
        level = level * one(*cut)
    return level


def scatter_about(stream_key, dims, deviation, limit, shards=(), kind=jnp.bfloat16):
    gain = level_of(stream_key, dims, shards, -0.22, 0.18) if shards else 1.0
    array = jax.random.normal(stream_key, dims, jnp.float32) * deviation * gain
    return jnp.minimum(jnp.maximum(array, -limit), limit).astype(kind)


def setup_inputs(seed: int = 0) -> dict:
    seeds = jax.random.split(jax.random.key(seed), 7)
    return {
        "wavefunction": scatter_about(seeds[0], (SECTORS, B, B), 1.0, 6.0, ((0, 8), (1, 32))),
        "left_ops": scatter_about(seeds[1], (SECTORS, TERMS, B, B), (B * TERMS) ** -0.5, 0.0234375, ((0, 8), (1, 32))),
        "right_ops": scatter_about(seeds[2], (SECTORS, TERMS, B, B), B ** -0.5, 0.21875, ((0, 8), (1, 32))),
        "diagonal": draw_diagonal(jax.random.fold_in(seeds[6], 71), 0),
        "sector_sizes": touch_ends(jax.random.randint(seeds[4], (SECTORS,), B // 4, B + 1), jax.random.fold_in(seeds[4], 1), B // 4, B).astype(jnp.int32),
        "partner": draw_partner(jax.random.fold_in(seeds[6], 71), 0),
    }


def reference(wavefunction, left_ops, right_ops, diagonal, sector_sizes, partner):
    positions = jnp.arange(B, dtype=jnp.int32)
    live_mask = (positions[None, :, None] < sector_sizes[:, None, None]) & (positions[None, None, :] < sector_sizes[:, None, None])
    live = jnp.where(live_mask, wavefunction, jnp.zeros_like(wavefunction))

    def sector_step(carried, sector):
        direct_all, adjoint_all = carried
        other = partner[sector]
        left_float = left_ops[sector].astype(jnp.float32)
        right_float = right_ops[sector].astype(jnp.float32)
        forward = jnp.einsum('kab,bc->kac', left_float, live[other].astype(jnp.float32)).astype(jnp.bfloat16)
        direct_term = jnp.einsum('kac,kdc->ad', forward.astype(jnp.float32), right_float)
        backward = jnp.einsum('kba,bc->kac', left_float, live[sector].astype(jnp.float32)).astype(jnp.bfloat16)
        adjoint_term = jnp.einsum('kac,kcd->ad', backward.astype(jnp.float32), right_float)
        direct_all = direct_all.at[sector].set(direct_term)
        adjoint_all = adjoint_all.at[other].add(adjoint_term)
        return (direct_all, adjoint_all), 0

    zero_blocks = jnp.zeros((SECTORS, B, B), jnp.float32)
    (direct_all, adjoint_all), _ = lax.scan(sector_step, (zero_blocks, zero_blocks), jnp.arange(SECTORS, dtype=jnp.int32))
    wave_float = live.astype(jnp.float32)
    sigma = jnp.where(live_mask, direct_all + adjoint_all + diagonal * wave_float, jnp.zeros_like(direct_all))
    energy = jnp.sum(wave_float * sigma) / jnp.sum(wave_float * wave_float)
    residual = sigma - energy * wave_float
    updated = wave_float - residual / jnp.maximum(jnp.abs(diagonal - energy), 1.0)
    return updated, residual
```

```python
import functools

import jax
import jax.numpy as jnp
from jax import lax
from jax.experimental import pallas as pl
from jax.experimental.pallas import tpu as pltpu
from jax.sharding import Mesh
from jax.sharding import PartitionSpec as P


SEC = ("sec_0", "sec_1")
OP = ("op_0", "op_1")
Y, Z = OP
bf16 = jnp.bfloat16
f32 = jnp.float32
VMEM = pl.BlockSpec(memory_space=pltpu.VMEM)
SMEM = pl.BlockSpec(memory_space=pltpu.SMEM)
NN = (((1,), (0,)), ((), ()))
TN = (((0,), (0,)), ((), ()))
NT = (((1,), (1,)), ((), ()))


def to_peers(value, axis):
    peers = lax.axis_size(axis)
    copies = jnp.broadcast_to(value[None], (peers, *value.shape))
    return lax.all_to_all(copies, axis, 0, 0, tiled=True)


def from_ahead(value, steps):
    peers = lax.axis_size(Y)
    return lax.ppermute(value, Y, [(i, (i - steps) % peers) for i in range(peers)])


def to_ahead(value, steps):
    peers = lax.axis_size(Y)
    return lax.ppermute(value, Y, [(i, (i + steps) % peers) for i in range(peers)])


def three_parts(total):
    high = total.astype(bf16)
    rest = total - high.astype(f32)
    middle = rest.astype(bf16)
    low = (rest - middle.astype(f32)).astype(bf16)
    return high, middle, low


def products(ahead, x_refs, left_ref, right_ref, x_all, half, first_dims, second_dims):
    count = len(x_refs)
    rows = x_refs[0].shape[0]
    terms, width, _ = left_ref.shape
    for step, ref in enumerate(x_refs):
        place = pl.multiple_of(lax.rem(ahead + step, count) * rows, rows)
        x_all[pl.ds(place, rows), :] = ref[...]
    for k in range(terms):
        first = lax.dot_general(
            left_ref[k], x_all[...], first_dims, preferred_element_type=f32
        ).astype(bf16)
        for block in range(count):
            place = pl.multiple_of(lax.rem(block - ahead + count, count) * rows, rows)
            half[pl.ds(place, rows), k * width : (k + 1) * width] = first[
                block * rows : (block + 1) * rows
            ]
    if second_dims == NN:
        right = right_ref[...].reshape(terms * width, width)
        return lax.dot_general(half[...], right, NN, preferred_element_type=f32)
    total = None
    for k in range(terms):
        part = lax.dot_general(
            half[:, k * width : (k + 1) * width],
            right_ref[k],
            second_dims,
            preferred_element_type=f32,
        )
        total = part if total is None else total + part
    return total


def adjoint_kernel(count, left_ref, right_ref, *refs):
    x_refs, outs, (x_all, half) = refs[:count], refs[count : 2 * count], refs[2 * count :]
    rows = x_refs[0].shape[0]
    total = products(lax.axis_index(Y), x_refs, left_ref, right_ref, x_all, half, TN, NN)
    for step in range(count):
        outs[step][...] = total[step * rows : (step + 1) * rows].astype(outs[step].dtype)


def direct_kernel(count, left_ref, right_ref, live_ref, diagonal_ref, *refs):
    x_refs, own_refs = refs[:count], refs[count : 2 * count]
    outs, sums_ref = refs[2 * count : 3 * count], refs[3 * count]
    x_all, half = refs[3 * count + 1 :]
    rows = x_refs[0].shape[0]
    total = products(lax.axis_index(Y), x_refs, left_ref, right_ref, x_all, half, NN, NT)
    wave = live_ref[...].astype(f32)
    square = wave * wave
    norm = jnp.sum(jnp.sum(square, axis=0, keepdims=True), axis=1, keepdims=True)
    mixed = jnp.sum(square * diagonal_ref[...], axis=0, keepdims=True)
    for step in range(count):
        block = total[step * rows : (step + 1) * rows]
        mixed += 2.0 * jnp.sum(own_refs[step][...].astype(f32) * block, axis=0, keepdims=True)
        if step == 0:
            outs[step][...] = block
        else:
            outs[step][:rows, :] = block.astype(bf16)
    mixed = jnp.sum(mixed, axis=1, keepdims=True)
    tile = sums_ref.shape
    row = lax.broadcasted_iota(jnp.int32, tile, 0)
    sums_ref[...] = jnp.where(
        row == 0, jnp.broadcast_to(mixed, tile), jnp.broadcast_to(norm, tile)
    )
    tail = (outs[1].shape[0] - rows, outs[1].shape[1])
    row = lax.broadcasted_iota(jnp.int32, tail, 0)
    extra = jnp.zeros(tail, f32)
    for place, part in enumerate(three_parts(mixed) + three_parts(norm)):
        extra = jnp.where(row == place, jnp.broadcast_to(part.astype(f32), tail), extra)
    extra = extra.astype(bf16)
    for step in range(1, count):
        outs[step][rows:, :] = extra


def tiles_of(rows, width):
    return [(r, c) for r in range(0, rows, 8) for c in range(0, width, 128)]


def row_sum_kernel(own_ref, *refs):
    others, out_ref = refs[:-1], refs[-1]
    rows, width = own_ref.shape
    peers = out_ref.shape[0]
    each = rows // peers
    for pair in range(0, peers, 2):
        part = slice(pair * each, (pair + 2) * each)
        total = own_ref[part, :]
        for ref in others:
            total += ref[part, :].astype(f32)
        for z in range(2):
            for n, (r, c) in enumerate(tiles_of(each, width)):
                out_ref[pair + z, 8 * n : 8 * n + 8, :] = total[
                    z * each + r : z * each + r + 8, c : c + 128
                ]


def row_sum_with_sums_kernel(own_ref, sums_ref, *refs):
    row_sum_kernel(own_ref, *refs)
    others, out_ref = refs[:-1], refs[-1]
    rows = own_ref.shape[0]
    tile = sums_ref[...]
    mixed, norm = tile[0:1, :], tile[1:2, :]
    for ref in others:
        extra = ref[rows:, 0:128].astype(f32)
        mixed += extra[0:1] + extra[1:2] + extra[2:3]
        norm += extra[3:4] + extra[4:5] + extra[5:6]
    row = lax.broadcasted_iota(jnp.int32, tile.shape, 0)
    whole = jnp.where(row == 0, mixed, norm)
    for z in range(out_ref.shape[0]):
        out_ref[z, out_ref.shape[1] - 8 :, :] = whole


def meet_kernel(adjoint_ref, direct_ref, send_ref, rows_ref):
    peers, length, _ = adjoint_ref.shape
    adjoint, direct = adjoint_ref[0], direct_ref[0]
    for z in range(1, peers):
        adjoint += adjoint_ref[z]
        direct += direct_ref[z]
    rows_ref[...] = direct[:length]
    for sector in range(send_ref.shape[0]):
        send_ref[sector, :length, :] = adjoint
        send_ref[sector, length:, :] = direct[length:]


def update_kernel(
    partner_ref, size_ref, got_ref, direct_ref, diagonal_ref, live_ref, updated_ref, residual_ref
):
    rows, width = live_ref.shape
    length = direct_ref.shape[0]
    sectors = got_ref.shape[0]
    me = lax.axis_index(SEC)
    source = jnp.int32(0)
    sums = got_ref[0, length:, :]
    for sector in range(sectors):
        source = jnp.where(partner_ref[sector] == me, sector, source)
        if sector:
            sums += got_ref[sector, length:, :]
    energy = sums[0:1, :] / sums[1:2, :]
    size = size_ref[0]
    base = lax.axis_index(OP) * rows
    for n, (r, c) in enumerate(tiles_of(rows, width)):
        where_row = base + r + lax.broadcasted_iota(jnp.int32, (8, 128), 0)
        where_col = c + lax.broadcasted_iota(jnp.int32, (8, 128), 1)
        wave = live_ref[r : r + 8, c : c + 128].astype(f32)
        diagonal = diagonal_ref[r : r + 8, c : c + 128]
        part = slice(8 * n, 8 * n + 8)
        sigma = direct_ref[part, :] + got_ref[source, part, :] + diagonal * wave
        sigma = jnp.where((where_row < size) & (where_col < size), sigma, 0.0)
        residual = sigma - energy * wave
        residual_ref[r : r + 8, c : c + 128] = residual
        updated_ref[r : r + 8, c : c + 128] = wave - residual / jnp.maximum(
            jnp.abs(diagonal - energy), 1.0
        )


def run(kernel, name, outs, specs, scratch=(), flops=0, bytes_accessed=2**20, limit=16):
    return pl.pallas_call(
        kernel,
        out_shape=outs,
        in_specs=specs,
        out_specs=jax.tree.map(lambda _: VMEM, outs),
        scratch_shapes=list(scratch),
        compiler_params=pltpu.CompilerParams(vmem_limit_bytes=limit * 2**20),
        cost_estimate=pl.CostEstimate(
            flops=flops, bytes_accessed=bytes_accessed, transcendentals=0
        ),
        name=name,
    )


def per_device(wavefunction, left_ops, right_ops, diagonal, sector_sizes, partner):
    _, rows, width = wavefunction.shape
    terms = left_ops.shape[1]
    lines, peers = lax.axis_size(Y), lax.axis_size(Z)
    sectors = lax.axis_size(SEC)
    me = lax.axis_index(SEC)
    base = lax.axis_index(OP) * rows
    size = sector_sizes[0]
    row_index = base + lax.broadcasted_iota(jnp.int32, (rows, width), 0)
    col_index = lax.broadcasted_iota(jnp.int32, (rows, width), 1)
    wave = wavefunction[0]
    live = jnp.where((row_index < size) & (col_index < size), wave, jnp.zeros_like(wave))
    left, right, diag = left_ops[0], right_ops[0], diagonal[0]
    block = peers * rows

    own = to_peers(live, Z).reshape(block, width)
    every = to_peers(live, SEC).reshape(sectors, rows, width)
    other = lax.dynamic_index_in_dim(every, partner[me], 0, keepdims=False)
    theirs = to_peers(other, Z).reshape(block, width)

    own_parts = [own] + [from_ahead(own, n) for n in range(1, lines)]
    their_parts = [theirs] + [from_ahead(theirs, n) for n in range(1, lines)]

    flops = 4 * terms * width**3
    scratch = [pltpu.VMEM((width, width), bf16), pltpu.VMEM((width, terms * width), bf16)]
    whole = jax.ShapeDtypeStruct((block, width), f32)
    sent = jax.ShapeDtypeStruct((block, width), bf16)
    longer = jax.ShapeDtypeStruct((block + 16, width), bf16)
    tile = jax.ShapeDtypeStruct((8, 128), f32)
    adjoint = run(
        functools.partial(adjoint_kernel, lines),
        "adjoint",
        [whole] + [sent] * (lines - 1),
        [VMEM] * (2 + lines),
        scratch,
        flops,
        limit=40,
    )(left, right, *own_parts)
    direct = run(
        functools.partial(direct_kernel, lines),
        "direct",
        [whole] + [longer] * (lines - 1) + [tile],
        [VMEM] * (4 + 2 * lines),
        scratch,
        flops,
        limit=40,
    )(left, right, live, diag, *their_parts, *own_parts)

    length = rows * width // 128
    adjoint_got = [to_ahead(adjoint[n], n) for n in range(1, lines)]
    adjoint_lines = run(
        row_sum_kernel,
        "adjoint_rows",
        jax.ShapeDtypeStruct((peers, length, 128), f32),
        [VMEM] * lines,
    )(adjoint[0], *adjoint_got)
    direct_got = [to_ahead(direct[n], n) for n in range(1, lines)]
    direct_lines = run(
        row_sum_with_sums_kernel,
        "direct_rows",
        jax.ShapeDtypeStruct((peers, length + 8, 128), f32),
        [VMEM] * (1 + lines),
    )(direct[0], direct[lines], *direct_got)
    adjoint_rows = lax.all_to_all(adjoint_lines, Z, 0, 0, tiled=True)
    direct_rows = lax.all_to_all(direct_lines, Z, 0, 0, tiled=True)
    send, mine = run(
        meet_kernel,
        "meet",
        [
            jax.ShapeDtypeStruct((sectors, length + 8, 128), f32),
            jax.ShapeDtypeStruct((length, 128), f32),
        ],
        [VMEM] * 2,
    )(adjoint_rows, direct_rows)
    got = lax.all_to_all(send, SEC, 0, 0, tiled=True)
    result = jax.ShapeDtypeStruct((rows, width), f32)
    updated, residual = run(
        update_kernel, "update", [result, result], [SMEM, SMEM] + [VMEM] * 4
    )(partner, sector_sizes, got, mine, diag, live)
    return updated[None], residual[None]


def solution(mesh):
    finer = Mesh(mesh.devices.reshape(4, 2, 4, 8), SEC + OP)
    return jax.shard_map(
        per_device,
        mesh=finer,
        in_specs=(
            P(SEC, OP, None),
            P(SEC, OP, None, None),
            P(SEC, OP, None, None),
            P(SEC, OP, None),
            P(SEC),
            P(),
        ),
        out_specs=(P(SEC, OP, None), P(SEC, OP, None)),
        check_vma=False,
    )
```

```python
import functools

import jax
import jax.numpy as jnp
from jax import lax
from jax.experimental import pallas as pl
from jax.experimental.pallas import tpu as pltpu
from jax.sharding import Mesh
from jax.sharding import PartitionSpec as P


SEC = ("sec_0", "sec_1")
OP = ("op_0", "op_1")
Y, Z = OP
bf16 = jnp.bfloat16
f32 = jnp.float32
VMEM = pl.BlockSpec(memory_space=pltpu.VMEM)
SMEM = pl.BlockSpec(memory_space=pltpu.SMEM)
HBM = pl.BlockSpec(memory_space=pltpu.HBM)
NN = (((1,), (0,)), ((), ()))
TN = (((0,), (0,)), ((), ()))
NT = (((1,), (1,)), ((), ()))


def other_sectors():
    far, near = (lax.axis_size(name) for name in SEC)
    return [(i, j) for i in range(far) for j in range(near) if i or j]


def from_sector(value, step):
    far, near = (lax.axis_size(name) for name in SEC)
    pairs = [
        (i * near + j, (i + step[0]) % far * near + (j + step[1]) % near)
        for i in range(far)
        for j in range(near)
    ]
    return lax.ppermute(value, SEC, pairs)


def sector_behind(step):
    far, near = (lax.axis_size(name) for name in SEC)
    i = lax.rem(lax.axis_index(SEC[0]) - step[0] + far, far)
    j = lax.rem(lax.axis_index(SEC[1]) - step[1] + near, near)
    return i * near + j


def from_ahead(value, steps):
    peers = lax.axis_size(Y)
    return lax.ppermute(value, Y, [(i, (i - steps) % peers) for i in range(peers)])


def to_ahead(value, steps):
    peers = lax.axis_size(Y)
    return lax.ppermute(value, Y, [(i, (i + steps) % peers) for i in range(peers)])


def live_kernel(size_ref, wave_ref, live_ref, copies_ref):
    rows, width = wave_ref.shape
    size = size_ref[0]
    row = lax.axis_index(OP) * rows + lax.broadcasted_iota(jnp.int32, (rows, width), 0)
    col = lax.broadcasted_iota(jnp.int32, (rows, width), 1)
    wave = wave_ref[...].astype(f32)
    live = jnp.where((row < size) & (col < size), wave, 0.0).astype(bf16)
    live_ref[...] = live
    for z in range(copies_ref.shape[0]):
        copies_ref[z] = live


def choose_kernel(steps, partner_ref, live_ref, *refs):
    got_refs, copies_ref = refs[:-1], refs[-1]
    partner = partner_ref[lax.axis_index(SEC)]

    def place(ref):
        value = ref[...]
        for z in range(copies_ref.shape[0]):
            copies_ref[z] = value

    @pl.when(partner == lax.axis_index(SEC))
    def _():
        place(live_ref)

    for step, ref in zip(steps, got_refs):

        @pl.when(partner == sector_behind(step))
        def _(ref=ref):
            place(ref)


def products(x_refs, operators, outs, scratch, first_dims, second_dims):
    left_hbm, right_hbm = operators
    x_all, half, left_ref, right_ref, arrived = scratch
    count = len(x_refs)
    ahead = lax.axis_index(Y)
    rows = x_refs[0].shape[0]
    terms, width, _ = left_ref.shape
    copies = [
        pltpu.make_async_copy(hbm.at[k], ref.at[k], arrived.at[n, k])
        for n, (hbm, ref) in enumerate(((left_hbm, left_ref), (right_hbm, right_ref)))
        for k in range(terms)
    ]
    copies[0].start()
    copies[1].start()
    for step, ref in enumerate(x_refs):
        place = pl.multiple_of(lax.rem(ahead + step, count) * rows, rows)
        x_all[pl.ds(place, rows), :] = ref[...]
    for k in range(terms):
        copies[k].wait()
        for later in copies[2 * k + 2 : 2 * k + 4]:
            later.start()
        first = lax.dot_general(
            left_ref[k], x_all[...], first_dims, preferred_element_type=f32
        ).astype(bf16)
        for block in range(count):
            place = pl.multiple_of(lax.rem(block - ahead + count, count) * rows, rows)
            half[pl.ds(place, rows), k * width : (k + 1) * width] = first[
                block * rows : (block + 1) * rows
            ]
    for copy in copies[terms:]:
        copy.wait()
    if second_dims == NN:
        right = right_ref[...].reshape(terms * width, width)
        total = lax.dot_general(half[...], right, NN, preferred_element_type=f32)
    else:
        total = None
        for k in range(terms):
            part = lax.dot_general(
                half[:, k * width : (k + 1) * width],
                right_ref[k],
                second_dims,
                preferred_element_type=f32,
            )
            total = part if total is None else total + part
    for step in range(count):
        outs[step][...] = total[step * rows : (step + 1) * rows].astype(outs[step].dtype)


def adjoint_kernel(count, left_hbm, right_hbm, *refs):
    products(
        refs[:count], (left_hbm, right_hbm), refs[count : 2 * count], refs[2 * count :], TN, NN
    )


def direct_kernel(count, left_hbm, right_hbm, *refs):
    products(
        refs[:count], (left_hbm, right_hbm), refs[count : 2 * count], refs[2 * count :], NN, NT
    )


def sums_kernel(count, live_ref, diagonal_ref, *refs):
    x_refs, adjoint_refs, sums_ref = refs[:count], refs[count : 2 * count], refs[2 * count]
    wave = live_ref[...].astype(f32)
    square = wave * wave
    norm = jnp.sum(square, axis=0, keepdims=True)
    mixed = jnp.sum(square * diagonal_ref[...], axis=0, keepdims=True)
    for x_ref, adjoint_ref in zip(x_refs, adjoint_refs):
        pair = x_ref[...].astype(f32) * adjoint_ref[...].astype(f32)
        mixed += 2.0 * jnp.sum(pair, axis=0, keepdims=True)
    mixed = jnp.sum(mixed, axis=1, keepdims=True)
    norm = jnp.sum(norm, axis=1, keepdims=True)
    tile = sums_ref.shape
    row = lax.broadcasted_iota(jnp.int32, tile, 0)
    sums_ref[...] = jnp.where(
        row == 0, jnp.broadcast_to(mixed, tile), jnp.broadcast_to(norm, tile)
    )


def tiles_of(rows, width):
    return [(r, c) for r in range(0, rows, 8) for c in range(0, width, 128)]


def rows_kernel(count, *refs):
    blocks, sums_refs, out_ref = refs[:count], refs[count:-1], refs[-1]
    rows, width = blocks[0].shape
    peers = out_ref.shape[0]
    each = rows // peers
    for pair in range(0, peers, 2):
        part = slice(pair * each, (pair + 2) * each)
        total = blocks[0][part, :].astype(f32)
        for ref in blocks[1:]:
            total += ref[part, :].astype(f32)
        for z in range(2):
            for n, (r, c) in enumerate(tiles_of(each, width)):
                out_ref[pair + z, 8 * n : 8 * n + 8, :] = total[
                    z * each + r : z * each + r + 8, c : c + 128
                ]
    if sums_refs:
        total = sums_refs[0][...]
        for ref in sums_refs[1:]:
            total += ref[...]
        for z in range(peers):
            out_ref[z, out_ref.shape[1] - 8 :, :] = total


def meet_kernel(got_ref, out_ref):
    total = got_ref[0]
    for z in range(1, got_ref.shape[0]):
        total += got_ref[z]
    out_ref[...] = total


def update_kernel(
    steps, partner_ref, size_ref, direct_ref, diagonal_ref, live_ref, *refs
):
    got_refs, (updated_ref, residual_ref, routed) = refs[:-3], refs[-3:]
    rows, width = live_ref.shape
    peers, length, _ = direct_ref.shape
    me = lax.axis_index(SEC)
    sums = None
    for step, got_ref in zip([(0, 0)] + steps, got_refs):
        part = got_ref[length:, :]
        sums = part if sums is None else sums + part

        @pl.when(partner_ref[sector_behind(step)] == me)
        def _(got_ref=got_ref):
            routed[...] = got_ref[:length, :]

    energy = sums[0:1, :] / sums[1:2, :]
    size = size_ref[0]
    base = lax.axis_index(OP) * rows
    for n, (r, c) in enumerate(tiles_of(rows, width)):
        where_row = base + r + lax.broadcasted_iota(jnp.int32, (8, 128), 0)
        where_col = c + lax.broadcasted_iota(jnp.int32, (8, 128), 1)
        wave = live_ref[r : r + 8, c : c + 128].astype(f32)
        diagonal = diagonal_ref[r : r + 8, c : c + 128]
        part = slice(8 * n, 8 * n + 8)
        direct = direct_ref[0, part, :]
        for z in range(1, peers):
            direct += direct_ref[z, part, :]
        sigma = direct + routed[part, :] + diagonal * wave
        sigma = jnp.where((where_row < size) & (where_col < size), sigma, 0.0)
        residual = sigma - energy * wave
        residual_ref[r : r + 8, c : c + 128] = residual
        updated_ref[r : r + 8, c : c + 128] = wave - residual / jnp.maximum(
            jnp.abs(diagonal - energy), 1.0
        )


def run(kernel, name, outs, specs, scratch=(), flops=0, bytes_accessed=2**20, limit=16):
    return pl.pallas_call(
        kernel,
        out_shape=outs,
        in_specs=specs,
        out_specs=jax.tree.map(lambda _: VMEM, outs),
        scratch_shapes=list(scratch),
        compiler_params=pltpu.CompilerParams(vmem_limit_bytes=limit * 2**20),
        cost_estimate=pl.CostEstimate(
            flops=flops, bytes_accessed=bytes_accessed, transcendentals=0
        ),
        name=name,
    )


def per_device(wavefunction, left_ops, right_ops, diagonal, sector_sizes, partner):
    _, rows, width = wavefunction.shape
    terms = left_ops.shape[1]
    lines, peers = lax.axis_size(Y), lax.axis_size(Z)
    left, right, diag = left_ops[0], right_ops[0], diagonal[0]
    block = peers * rows
    length = rows * width // 128
    around = range(1, lines)
    steps = other_sectors()

    def shape(*dims, dtype=f32):
        return jax.ShapeDtypeStruct(dims, dtype)

    live, copies = run(
        live_kernel,
        "live",
        [shape(rows, width, dtype=bf16), shape(peers, rows, width, dtype=bf16)],
        [SMEM, VMEM],
    )(sector_sizes, wavefunction[0])
    own = lax.all_to_all(copies, Z, 0, 0, tiled=True).reshape(block, width)
    others = [from_sector(live, step) for step in steps]
    copies = run(
        functools.partial(choose_kernel, steps),
        "choose",
        shape(peers, rows, width, dtype=bf16),
        [SMEM] + [VMEM] * (1 + len(steps)),
    )(partner, live, *others)
    theirs = lax.all_to_all(copies, Z, 0, 0, tiled=True).reshape(block, width)
    own_parts = [own] + [from_ahead(own, n) for n in around]
    their_parts = [theirs] + [from_ahead(theirs, n) for n in around]

    flops = 4 * terms * width**3
    scratch = [
        pltpu.VMEM((width, width), bf16),
        pltpu.VMEM((width, terms * width), bf16),
        pltpu.VMEM((terms, width, width), bf16),
        pltpu.VMEM((terms, width, width), bf16),
        pltpu.SemaphoreType.DMA((2, terms)),
    ]
    outs = [shape(block, width)] + [shape(block, width, dtype=bf16)] * (lines - 1)
    specs = [HBM, HBM] + [VMEM] * lines
    adjoint = run(
        functools.partial(adjoint_kernel, lines), "adjoint", outs, specs, scratch, flops, limit=48
    )(left, right, *own_parts)
    adjoint_got = [to_ahead(adjoint[n], n) for n in around]
    sums = run(
        functools.partial(sums_kernel, lines), "sums", shape(8, 128), [VMEM] * (2 + 2 * lines)
    )(live, diag, *their_parts, *adjoint)
    sums_got = [to_ahead(sums, n) for n in around]
    direct = run(
        functools.partial(direct_kernel, lines), "direct", outs, specs, scratch, flops, limit=48
    )(left, right, *their_parts)
    direct_got = [to_ahead(direct[n], n) for n in around]

    adjoint_lines = run(
        functools.partial(rows_kernel, lines),
        "adjoint_rows",
        shape(peers, length + 8, 128),
        [VMEM] * (2 * lines),
    )(adjoint[0], *adjoint_got, sums, *sums_got)
    adjoint_mine = run(meet_kernel, "meet", shape(length + 8, 128), [VMEM])(
        lax.all_to_all(adjoint_lines, Z, 0, 0, tiled=True)
    )
    routed = [adjoint_mine] + [from_sector(adjoint_mine, step) for step in steps]
    direct_lines = run(
        functools.partial(rows_kernel, lines),
        "direct_rows",
        shape(peers, length, 128),
        [VMEM] * lines,
    )(direct[0], *direct_got)
    direct_mine = lax.all_to_all(direct_lines, Z, 0, 0, tiled=True)
    updated, residual = run(
        functools.partial(update_kernel, steps),
        "update",
        [shape(rows, width)] * 2,
        [SMEM, SMEM] + [VMEM] * (3 + len(routed)),
        [pltpu.VMEM((length, 128), f32)],
    )(partner, sector_sizes, direct_mine, diag, live, *routed)
    return updated[None], residual[None]


def solution(mesh):
    finer = Mesh(mesh.devices.reshape(4, 2, 4, 8), SEC + OP)
    return jax.shard_map(
        per_device,
        mesh=finer,
        in_specs=(
            P(SEC, OP, None),
            P(SEC, OP, None, None),
            P(SEC, OP, None, None),
            P(SEC, OP, None),
            P(SEC),
            P(),
        ),
        out_specs=(P(SEC, OP, None), P(SEC, OP, None)),
        check_vma=False,
    )
```

```python
import functools

import jax
import jax.numpy as jnp
from jax import lax
from jax.experimental import pallas as pl
from jax.experimental.pallas import tpu as pltpu
from jax.sharding import Mesh
from jax.sharding import PartitionSpec as P


SEC = ("sec_0", "sec_1")
OP = ("op_0", "op_1")
Y, Z = OP
bf16 = jnp.bfloat16
f32 = jnp.float32
VMEM = pl.BlockSpec(memory_space=pltpu.VMEM)
SMEM = pl.BlockSpec(memory_space=pltpu.SMEM)
HBM = pl.BlockSpec(memory_space=pltpu.HBM)
NN = (((1,), (0,)), ((), ()))
TN = (((0,), (0,)), ((), ()))
NT = (((1,), (1,)), ((), ()))


def other_sectors():
    far, near = (lax.axis_size(name) for name in SEC)
    return [(i, j) for i in range(far) for j in range(near) if i or j]


def from_sector(value, step):
    far, near = (lax.axis_size(name) for name in SEC)
    pairs = [
        (i * near + j, (i + step[0]) % far * near + (j + step[1]) % near)
        for i in range(far)
        for j in range(near)
    ]
    return lax.ppermute(value, SEC, pairs)


def sector_behind(step):
    far, near = (lax.axis_size(name) for name in SEC)
    i = lax.rem(lax.axis_index(SEC[0]) - step[0] + far, far)
    j = lax.rem(lax.axis_index(SEC[1]) - step[1] + near, near)
    return i * near + j


def from_ahead(value, steps):
    peers = lax.axis_size(Y)
    return lax.ppermute(value, Y, [(i, (i - steps) % peers) for i in range(peers)])


def to_ahead(value, steps):
    peers = lax.axis_size(Y)
    return lax.ppermute(value, Y, [(i, (i + steps) % peers) for i in range(peers)])


def along_y(move, values):
    moved = []
    for n, value in enumerate(values, 1):
        moved.append(move(value, n))
    return moved


def live_kernel(size_ref, wave_ref, live_ref, copies_ref):
    rows, width = wave_ref.shape
    size = size_ref[0]
    row = lax.axis_index(OP) * rows + lax.broadcasted_iota(jnp.int32, (rows, width), 0)
    col = lax.broadcasted_iota(jnp.int32, (rows, width), 1)
    wave = wave_ref[...].astype(f32)
    live = jnp.where((row < size) & (col < size), wave, 0.0).astype(bf16)
    live_ref[...] = live
    for z in range(copies_ref.shape[0]):
        copies_ref[z] = live


def choose_kernel(steps, partner_ref, live_ref, *refs):
    got_refs, copies_ref = refs[:-1], refs[-1]
    partner = partner_ref[lax.axis_index(SEC)]

    def place(ref):
        value = ref[...]
        for z in range(copies_ref.shape[0]):
            copies_ref[z] = value

    @pl.when(partner == lax.axis_index(SEC))
    def _():
        place(live_ref)

    for step, ref in zip(steps, got_refs):

        @pl.when(partner == sector_behind(step))
        def _(ref=ref):
            place(ref)


def products(x_refs, operators, outs, scratch, first_dims, second_dims):
    left_hbm, right_hbm = operators
    x_all, half, left_ref, right_ref, arrived = scratch
    count = len(x_refs)
    ahead = lax.axis_index(Y)
    rows = x_refs[0].shape[0]
    terms, width, _ = left_ref.shape
    copies = [
        pltpu.make_async_copy(hbm.at[k], ref.at[k], arrived.at[n, k])
        for n, (hbm, ref) in enumerate(((left_hbm, left_ref), (right_hbm, right_ref)))
        for k in range(terms)
    ]
    copies[0].start()
    copies[1].start()
    for step, ref in enumerate(x_refs):
        place = pl.multiple_of(lax.rem(ahead + step, count) * rows, rows)
        x_all[pl.ds(place, rows), :] = ref[...]
    for k in range(terms):
        copies[k].wait()
        for later in copies[2 * k + 2 : 2 * k + 4]:
            later.start()
        first = lax.dot_general(
            left_ref[k], x_all[...], first_dims, preferred_element_type=f32
        ).astype(bf16)
        for block in range(count):
            place = pl.multiple_of(lax.rem(block - ahead + count, count) * rows, rows)
            half[pl.ds(place, rows), k * width : (k + 1) * width] = first[
                block * rows : (block + 1) * rows
            ]
    for copy in copies[terms:]:
        copy.wait()
    if second_dims == NN:
        right = right_ref[...].reshape(terms * width, width)
        total = lax.dot_general(half[...], right, NN, preferred_element_type=f32)
    else:
        total = None
        for k in range(terms):
            part = lax.dot_general(
                half[:, k * width : (k + 1) * width],
                right_ref[k],
                second_dims,
                preferred_element_type=f32,
            )
            total = part if total is None else total + part
    for step in range(count):
        outs[step][...] = total[step * rows : (step + 1) * rows].astype(outs[step].dtype)


def adjoint_kernel(count, left_hbm, right_hbm, *refs):
    products(
        refs[:count], (left_hbm, right_hbm), refs[count : 2 * count], refs[2 * count :], TN, NN
    )


def direct_kernel(count, left_hbm, right_hbm, *refs):
    products(
        refs[:count], (left_hbm, right_hbm), refs[count : 2 * count], refs[2 * count :], NN, NT
    )


def sums_kernel(count, live_ref, diagonal_ref, *refs):
    x_refs, adjoint_refs, sums_ref = refs[:count], refs[count : 2 * count], refs[2 * count]
    wave = live_ref[...].astype(f32)
    square = wave * wave
    norm = jnp.sum(square, axis=0, keepdims=True)
    mixed = jnp.sum(square * diagonal_ref[...], axis=0, keepdims=True)
    for x_ref, adjoint_ref in zip(x_refs, adjoint_refs):
        pair = x_ref[...].astype(f32) * adjoint_ref[...].astype(f32)
        mixed += 2.0 * jnp.sum(pair, axis=0, keepdims=True)
    mixed = jnp.sum(mixed, axis=1, keepdims=True)
    norm = jnp.sum(norm, axis=1, keepdims=True)
    tile = sums_ref.shape
    row = lax.broadcasted_iota(jnp.int32, tile, 0)
    sums_ref[...] = jnp.where(
        row == 0, jnp.broadcast_to(mixed, tile), jnp.broadcast_to(norm, tile)
    )


def tiles_of(rows, width):
    return [(r, c) for r in range(0, rows, 8) for c in range(0, width, 128)]


def rows_kernel(count, *refs):
    blocks, sums_refs, out_ref = refs[:count], refs[count:-1], refs[-1]
    rows, width = blocks[0].shape
    peers = out_ref.shape[0]
    each = rows // peers
    for pair in range(0, peers, 2):
        part = slice(pair * each, (pair + 2) * each)
        total = blocks[0][part, :].astype(f32)
        for ref in blocks[1:]:
            total += ref[part, :].astype(f32)
        for z in range(2):
            for n, (r, c) in enumerate(tiles_of(each, width)):
                out_ref[pair + z, 8 * n : 8 * n + 8, :] = total[
                    z * each + r : z * each + r + 8, c : c + 128
                ]
    if sums_refs:
        total = sums_refs[0][...]
        for ref in sums_refs[1:]:
            total += ref[...]
        for z in range(peers):
            out_ref[z, out_ref.shape[1] - 8 :, :] = total


def meet_kernel(got_ref, out_ref):
    total = got_ref[0]
    for z in range(1, got_ref.shape[0]):
        total += got_ref[z]
    out_ref[...] = total


def update_kernel(
    steps, partner_ref, size_ref, direct_ref, diagonal_ref, live_ref, *refs
):
    got_refs, (updated_ref, residual_ref, routed) = refs[:-3], refs[-3:]
    rows, width = live_ref.shape
    peers, length, _ = direct_ref.shape
    me = lax.axis_index(SEC)
    sums = None
    for step, got_ref in zip([(0, 0)] + steps, got_refs):
        part = got_ref[length:, :]
        sums = part if sums is None else sums + part

        @pl.when(partner_ref[sector_behind(step)] == me)
        def _(got_ref=got_ref):
            routed[...] = got_ref[:length, :]

    energy = sums[0:1, :] / sums[1:2, :]
    size = size_ref[0]
    base = lax.axis_index(OP) * rows
    for n, (r, c) in enumerate(tiles_of(rows, width)):
        where_row = base + r + lax.broadcasted_iota(jnp.int32, (8, 128), 0)
        where_col = c + lax.broadcasted_iota(jnp.int32, (8, 128), 1)
        wave = live_ref[r : r + 8, c : c + 128].astype(f32)
        diagonal = diagonal_ref[r : r + 8, c : c + 128]
        part = slice(8 * n, 8 * n + 8)
        direct = direct_ref[0, part, :]
        for z in range(1, peers):
            direct += direct_ref[z, part, :]
        sigma = direct + routed[part, :] + diagonal * wave
        sigma = jnp.where((where_row < size) & (where_col < size), sigma, 0.0)
        residual = sigma - energy * wave
        residual_ref[r : r + 8, c : c + 128] = residual
        updated_ref[r : r + 8, c : c + 128] = wave - residual / jnp.maximum(
            jnp.abs(diagonal - energy), 1.0
        )


def run(kernel, outs, specs, scratch=(), flops=0, bytes_accessed=2**20, limit=16):
    return pl.pallas_call(
        kernel,
        out_shape=outs,
        in_specs=specs,
        out_specs=jax.tree.map(lambda _: VMEM, outs),
        scratch_shapes=list(scratch),
        compiler_params=pltpu.CompilerParams(vmem_limit_bytes=limit * 2**20),
        cost_estimate=pl.CostEstimate(
            flops=flops, bytes_accessed=bytes_accessed, transcendentals=0
        ),
    )


def per_device(wavefunction, left_ops, right_ops, diagonal, sector_sizes, partner):
    _, rows, width = wavefunction.shape
    terms = left_ops.shape[1]
    lines, peers = lax.axis_size(Y), lax.axis_size(Z)
    left, right, diag = left_ops[0], right_ops[0], diagonal[0]
    block = peers * rows
    length = rows * width // 128
    steps = other_sectors()

    def shape(*dims, dtype=f32):
        return jax.ShapeDtypeStruct(dims, dtype)

    live, copies = run(
        live_kernel,
        [shape(rows, width, dtype=bf16), shape(peers, rows, width, dtype=bf16)],
        [SMEM, VMEM],
    )(sector_sizes, wavefunction[0])
    own = lax.all_to_all(copies, Z, 0, 0, tiled=True).reshape(block, width)
    others = []
    for step in steps:
        others.append(from_sector(live, step))
    copies = run(
        functools.partial(choose_kernel, steps),
        shape(peers, rows, width, dtype=bf16),
        [SMEM] + [VMEM] * (1 + len(steps)),
    )(partner, live, *others)
    theirs = lax.all_to_all(copies, Z, 0, 0, tiled=True).reshape(block, width)
    own_parts = [own] + along_y(from_ahead, [own] * (lines - 1))
    their_parts = [theirs] + along_y(from_ahead, [theirs] * (lines - 1))

    flops = 4 * terms * width**3
    scratch = [
        pltpu.VMEM((width, width), bf16),
        pltpu.VMEM((width, terms * width), bf16),
        pltpu.VMEM((terms, width, width), bf16),
        pltpu.VMEM((terms, width, width), bf16),
        pltpu.SemaphoreType.DMA((2, terms)),
    ]
    outs = [shape(block, width)] + [shape(block, width, dtype=bf16)] * (lines - 1)
    specs = [HBM, HBM] + [VMEM] * lines
    adjoint = run(
        functools.partial(adjoint_kernel, lines), outs, specs, scratch, flops, limit=50
    )(left, right, *own_parts)
    adjoint_got = along_y(to_ahead, adjoint[1:])
    sums = run(
        functools.partial(sums_kernel, lines), shape(8, 128), [VMEM] * (2 + 2 * lines)
    )(live, diag, *their_parts, *adjoint)
    sums_got = along_y(to_ahead, [sums] * (lines - 1))
    direct = run(
        functools.partial(direct_kernel, lines), outs, specs, scratch, flops, limit=50
    )(left, right, *their_parts)
    direct_got = along_y(to_ahead, direct[1:])

    adjoint_lines = run(
        functools.partial(rows_kernel, lines), shape(peers, length + 8, 128), [VMEM] * (2 * lines)
    )(adjoint[0], *adjoint_got, sums, *sums_got)
    adjoint_lines = lax.all_to_all(adjoint_lines, Z, 0, 0, tiled=True)
    adjoint_mine = run(meet_kernel, shape(length + 8, 128), [VMEM])(adjoint_lines)
    routed = [adjoint_mine] + [from_sector(adjoint_mine, step) for step in steps]
    direct_lines = run(
        functools.partial(rows_kernel, lines), shape(peers, length, 128), [VMEM] * lines
    )(direct[0], *direct_got)
    direct_mine = lax.all_to_all(direct_lines, Z, 0, 0, tiled=True)
    updated, residual = run(
        functools.partial(update_kernel, steps),
        [shape(rows, width)] * 2,
        [SMEM, SMEM] + [VMEM] * (3 + len(routed)),
        [pltpu.VMEM((length, 128), f32)],
    )(partner, sector_sizes, direct_mine, diag, live, *routed)
    return updated[None], residual[None]


def solution(mesh):
    finer = Mesh(mesh.devices.reshape(4, 2, 4, 8), SEC + OP)
    return jax.shard_map(
        per_device,
        mesh=finer,
        in_specs=(
            P(SEC, OP, None),
            P(SEC, OP, None, None),
            P(SEC, OP, None, None),
            P(SEC, OP, None),
            P(SEC),
            P(),
        ),
        out_specs=(P(SEC, OP, None), P(SEC, OP, None)),
        check_vma=False,
    )
```

```python
import functools

import jax
import jax.numpy as jnp
from jax import lax
from jax.experimental import pallas as pl
from jax.experimental.pallas import tpu as pltpu
from jax.sharding import Mesh
from jax.sharding import PartitionSpec as P


SEC = ("sec_0", "sec_1")
OP = ("op_0", "op_1")
Y, Z = OP
bf16 = jnp.bfloat16
f32 = jnp.float32
VMEM = pl.BlockSpec(memory_space=pltpu.VMEM)
SMEM = pl.BlockSpec(memory_space=pltpu.SMEM)
HBM = pl.BlockSpec(memory_space=pltpu.HBM)
NN = (((1,), (0,)), ((), ()))
TN = (((0,), (0,)), ((), ()))
NT = (((1,), (1,)), ((), ()))


def other_sectors():
    far, near = (lax.axis_size(name) for name in SEC)
    return [(i, j) for i in range(far) for j in range(near) if i or j]


def from_sector(value, step):
    far, near = (lax.axis_size(name) for name in SEC)
    pairs = [
        (i * near + j, (i + step[0]) % far * near + (j + step[1]) % near)
        for i in range(far)
        for j in range(near)
    ]
    return lax.ppermute(value, SEC, pairs)


def sector_behind(step):
    far, near = (lax.axis_size(name) for name in SEC)
    i = lax.rem(lax.axis_index(SEC[0]) - step[0] + far, far)
    j = lax.rem(lax.axis_index(SEC[1]) - step[1] + near, near)
    return i * near + j


def from_ahead(value, steps):
    peers = lax.axis_size(Y)
    return lax.ppermute(value, Y, [(i, (i - steps) % peers) for i in range(peers)])


def to_ahead(value, steps):
    peers = lax.axis_size(Y)
    return lax.ppermute(value, Y, [(i, (i + steps) % peers) for i in range(peers)])


def along_y(move, values):
    moved = []
    for n, value in enumerate(values, 1):
        moved.append(move(value, n))
    return moved


def live_kernel(size_ref, wave_ref, live_ref, copies_ref):
    rows, width = wave_ref.shape
    size = size_ref[0]
    row = lax.axis_index(OP) * rows + lax.broadcasted_iota(jnp.int32, (rows, width), 0)
    col = lax.broadcasted_iota(jnp.int32, (rows, width), 1)
    wave = wave_ref[...].astype(f32)
    live = jnp.where((row < size) & (col < size), wave, 0.0).astype(bf16)
    live_ref[...] = live
    for z in range(copies_ref.shape[0]):
        copies_ref[z] = live


def choose_kernel(steps, partner_ref, live_ref, *refs):
    got_refs, copies_ref = refs[:-1], refs[-1]
    partner = partner_ref[lax.axis_index(SEC)]

    def place(ref):
        value = ref[...]
        for z in range(copies_ref.shape[0]):
            copies_ref[z] = value

    @pl.when(partner == lax.axis_index(SEC))
    def _():
        place(live_ref)

    for step, ref in zip(steps, got_refs):

        @pl.when(partner == sector_behind(step))
        def _(ref=ref):
            place(ref)


def products(x_refs, operators, outs, scratch, first_dims, second_dims):
    left_hbm, right_hbm = operators
    x_all, half, left_ref, right_ref, arrived = scratch
    count = len(x_refs)
    ahead = lax.axis_index(Y)
    rows = x_refs[0].shape[0]
    terms, width, _ = left_ref.shape
    copies = []
    for k in range(terms):
        copies.append((left_hbm, left_ref, 0, k))
        if k:
            copies.append((right_hbm, right_ref, 1, k - 1))
    copies.append((right_hbm, right_ref, 1, terms - 1))
    copies = [
        pltpu.make_async_copy(hbm.at[k], ref.at[k], arrived.at[side, k])
        for hbm, ref, side, k in copies
    ]
    copies[0].start()
    copies[1].start()
    for step, ref in enumerate(x_refs):
        place = pl.multiple_of(lax.rem(ahead + step, count) * rows, rows)
        x_all[pl.ds(place, rows), :] = ref[...]
    total = None
    for n in range(2 * terms):
        copies[n].wait()
        if n + 2 < 2 * terms:
            copies[n + 2].start()
        if n == 0 or (n % 2 and n < 2 * terms - 1):
            k = (n + 1) // 2
            first = lax.dot_general(
                left_ref[k], x_all[...], first_dims, preferred_element_type=f32
            ).astype(bf16)
            for block in range(count):
                place = pl.multiple_of(lax.rem(block - ahead + count, count) * rows, rows)
                half[pl.ds(place, rows), k * width : (k + 1) * width] = first[
                    block * rows : (block + 1) * rows
                ]
        else:
            k = n // 2 - 1 if n < 2 * terms - 1 else terms - 1
            part = lax.dot_general(
                half[:, k * width : (k + 1) * width],
                right_ref[k],
                second_dims,
                preferred_element_type=f32,
            )
            total = part if total is None else total + part
    for step in range(count):
        outs[step][...] = total[step * rows : (step + 1) * rows].astype(outs[step].dtype)


def adjoint_kernel(count, left_hbm, right_hbm, *refs):
    products(
        refs[:count], (left_hbm, right_hbm), refs[count : 2 * count], refs[2 * count :], TN, NN
    )


def direct_kernel(count, left_hbm, right_hbm, *refs):
    products(
        refs[:count], (left_hbm, right_hbm), refs[count : 2 * count], refs[2 * count :], NN, NT
    )


def sums_kernel(count, live_ref, diagonal_ref, *refs):
    x_refs, adjoint_refs, sums_ref = refs[:count], refs[count : 2 * count], refs[2 * count]
    wave = live_ref[...].astype(f32)
    square = wave * wave
    norm = jnp.sum(square, axis=0, keepdims=True)
    mixed = jnp.sum(square * diagonal_ref[...], axis=0, keepdims=True)
    for x_ref, adjoint_ref in zip(x_refs, adjoint_refs):
        pair = x_ref[...].astype(f32) * adjoint_ref[...].astype(f32)
        mixed += 2.0 * jnp.sum(pair, axis=0, keepdims=True)
    mixed = jnp.sum(mixed, axis=1, keepdims=True)
    norm = jnp.sum(norm, axis=1, keepdims=True)
    tile = sums_ref.shape
    row = lax.broadcasted_iota(jnp.int32, tile, 0)
    sums_ref[...] = jnp.where(
        row == 0, jnp.broadcast_to(mixed, tile), jnp.broadcast_to(norm, tile)
    )


def tiles_of(rows, width):
    return [(r, c) for r in range(0, rows, 8) for c in range(0, width, 128)]


def rows_kernel(count, *refs):
    blocks, sums_refs, out_ref = refs[:count], refs[count:-1], refs[-1]
    rows, width = blocks[0].shape
    peers = out_ref.shape[0]
    each = rows // peers
    for pair in range(0, peers, 2):
        part = slice(pair * each, (pair + 2) * each)
        total = blocks[0][part, :].astype(f32)
        for ref in blocks[1:]:
            total += ref[part, :].astype(f32)
        for z in range(2):
            for n, (r, c) in enumerate(tiles_of(each, width)):
                out_ref[pair + z, 8 * n : 8 * n + 8, :] = total[
                    z * each + r : z * each + r + 8, c : c + 128
                ]
    if sums_refs:
        total = sums_refs[0][...]
        for ref in sums_refs[1:]:
            total += ref[...]
        for z in range(peers):
            out_ref[z, out_ref.shape[1] - 8 :, :] = total


def meet_kernel(got_ref, out_ref):
    total = got_ref[0]
    for z in range(1, got_ref.shape[0]):
        total += got_ref[z]
    out_ref[...] = total


def update_kernel(
    steps, partner_ref, size_ref, direct_ref, diagonal_ref, live_ref, *refs
):
    got_refs, (updated_ref, residual_ref, routed) = refs[:-3], refs[-3:]
    rows, width = live_ref.shape
    peers, length, _ = direct_ref.shape
    me = lax.axis_index(SEC)
    sums = None
    for step, got_ref in zip([(0, 0)] + steps, got_refs):
        part = got_ref[length:, :]
        sums = part if sums is None else sums + part

        @pl.when(partner_ref[sector_behind(step)] == me)
        def _(got_ref=got_ref):
            routed[...] = got_ref[:length, :]

    energy = sums[0:1, :] / sums[1:2, :]
    size = size_ref[0]
    base = lax.axis_index(OP) * rows
    for n, (r, c) in enumerate(tiles_of(rows, width)):
        where_row = base + r + lax.broadcasted_iota(jnp.int32, (8, 128), 0)
        where_col = c + lax.broadcasted_iota(jnp.int32, (8, 128), 1)
        wave = live_ref[r : r + 8, c : c + 128].astype(f32)
        diagonal = diagonal_ref[r : r + 8, c : c + 128]
        part = slice(8 * n, 8 * n + 8)
        direct = direct_ref[0, part, :]
        for z in range(1, peers):
            direct += direct_ref[z, part, :]
        sigma = direct + routed[part, :] + diagonal * wave
        sigma = jnp.where((where_row < size) & (where_col < size), sigma, 0.0)
        residual = sigma - energy * wave
        residual_ref[r : r + 8, c : c + 128] = residual
        updated_ref[r : r + 8, c : c + 128] = wave - residual / jnp.maximum(
            jnp.abs(diagonal - energy), 1.0
        )


def run(kernel, outs, specs, scratch=(), flops=0, bytes_accessed=2**20, limit=16):
    return pl.pallas_call(
        kernel,
        out_shape=outs,
        in_specs=specs,
        out_specs=jax.tree.map(lambda _: VMEM, outs),
        scratch_shapes=list(scratch),
        compiler_params=pltpu.CompilerParams(vmem_limit_bytes=limit * 2**20),
        cost_estimate=pl.CostEstimate(
            flops=flops, bytes_accessed=bytes_accessed, transcendentals=0
        ),
    )


def per_device(wavefunction, left_ops, right_ops, diagonal, sector_sizes, partner):
    _, rows, width = wavefunction.shape
    terms = left_ops.shape[1]
    lines, peers = lax.axis_size(Y), lax.axis_size(Z)
    left, right, diag = left_ops[0], right_ops[0], diagonal[0]
    block = peers * rows
    length = rows * width // 128
    steps = other_sectors()

    def shape(*dims, dtype=f32):
        return jax.ShapeDtypeStruct(dims, dtype)

    live, copies = run(
        live_kernel,
        [shape(rows, width, dtype=bf16), shape(peers, rows, width, dtype=bf16)],
        [SMEM, VMEM],
    )(sector_sizes, wavefunction[0])
    own = lax.all_to_all(copies, Z, 0, 0, tiled=True).reshape(block, width)
    others = []
    for step in steps:
        others.append(from_sector(live, step))
    copies = run(
        functools.partial(choose_kernel, steps),
        shape(peers, rows, width, dtype=bf16),
        [SMEM] + [VMEM] * (1 + len(steps)),
    )(partner, live, *others)
    theirs = lax.all_to_all(copies, Z, 0, 0, tiled=True).reshape(block, width)
    own_parts = [own] + along_y(from_ahead, [own] * (lines - 1))
    their_parts = [theirs] + along_y(from_ahead, [theirs] * (lines - 1))

    flops = 4 * terms * width**3
    scratch = [
        pltpu.VMEM((width, width), bf16),
        pltpu.VMEM((width, terms * width), bf16),
        pltpu.VMEM((terms, width, width), bf16),
        pltpu.VMEM((terms, width, width), bf16),
        pltpu.SemaphoreType.DMA((2, terms)),
    ]
    outs = [shape(block, width)] + [shape(block, width, dtype=bf16)] * (lines - 1)
    specs = [HBM, HBM] + [VMEM] * lines
    adjoint = run(
        functools.partial(adjoint_kernel, lines), outs, specs, scratch, flops, limit=50
    )(left, right, *own_parts)
    adjoint_got = along_y(to_ahead, adjoint[1:])
    sums = run(
        functools.partial(sums_kernel, lines), shape(8, 128), [VMEM] * (2 + 2 * lines)
    )(live, diag, *their_parts, *adjoint)
    sums_got = along_y(to_ahead, [sums] * (lines - 1))
    direct = run(
        functools.partial(direct_kernel, lines), outs, specs, scratch, flops, limit=50
    )(left, right, *their_parts)
    direct_got = along_y(to_ahead, direct[1:])

    adjoint_lines = run(
        functools.partial(rows_kernel, lines), shape(peers, length + 8, 128), [VMEM] * (2 * lines)
    )(adjoint[0], *adjoint_got, sums, *sums_got)
    adjoint_lines = lax.all_to_all(adjoint_lines, Z, 0, 0, tiled=True)
    adjoint_mine = run(meet_kernel, shape(length + 8, 128), [VMEM])(adjoint_lines)
    routed = [adjoint_mine] + [from_sector(adjoint_mine, step) for step in steps]
    direct_lines = run(
        functools.partial(rows_kernel, lines), shape(peers, length, 128), [VMEM] * lines
    )(direct[0], *direct_got)
    direct_mine = lax.all_to_all(direct_lines, Z, 0, 0, tiled=True)
    updated, residual = run(
        functools.partial(update_kernel, steps),
        [shape(rows, width)] * 2,
        [SMEM, SMEM] + [VMEM] * (3 + len(routed)),
        [pltpu.VMEM((length, 128), f32)],
    )(partner, sector_sizes, direct_mine, diag, live, *routed)
    return updated[None], residual[None]


def solution(mesh):
    finer = Mesh(mesh.devices.reshape(4, 2, 4, 8), SEC + OP)
    return jax.shard_map(
        per_device,
        mesh=finer,
        in_specs=(
            P(SEC, OP, None),
            P(SEC, OP, None, None),
            P(SEC, OP, None, None),
            P(SEC, OP, None),
            P(SEC),
            P(),
        ),
        out_specs=(P(SEC, OP, None), P(SEC, OP, None)),
        check_vma=False,
    )
```

```python
import functools

import jax
import jax.numpy as jnp
from jax import lax
from jax.experimental import pallas as pl
from jax.experimental.pallas import tpu as pltpu
from jax.sharding import Mesh
from jax.sharding import PartitionSpec as P


SEC = ("sec_0", "sec_1")
OP = ("op_0", "op_1")
Y, Z = OP
bf16 = jnp.bfloat16
f32 = jnp.float32
VMEM = pl.BlockSpec(memory_space=pltpu.VMEM)
SMEM = pl.BlockSpec(memory_space=pltpu.SMEM)
HBM = pl.BlockSpec(memory_space=pltpu.HBM)
NN = (((1,), (0,)), ((), ()))
TN = (((0,), (0,)), ((), ()))
NT = (((1,), (1,)), ((), ()))


def other_sectors():
    far, near = (lax.axis_size(name) for name in SEC)
    return [(i, j) for i in range(far) for j in range(near) if i or j]


def from_sector(value, step):
    far, near = (lax.axis_size(name) for name in SEC)
    pairs = [
        (i * near + j, (i + step[0]) % far * near + (j + step[1]) % near)
        for i in range(far)
        for j in range(near)
    ]
    return lax.ppermute(value, SEC, pairs)


def sector_behind(step):
    far, near = (lax.axis_size(name) for name in SEC)
    i = lax.rem(lax.axis_index(SEC[0]) - step[0] + far, far)
    j = lax.rem(lax.axis_index(SEC[1]) - step[1] + near, near)
    return i * near + j


def from_ahead(value, steps):
    peers = lax.axis_size(Y)
    return lax.ppermute(value, Y, [(i, (i - steps) % peers) for i in range(peers)])


def to_ahead(value, steps):
    peers = lax.axis_size(Y)
    return lax.ppermute(value, Y, [(i, (i + steps) % peers) for i in range(peers)])


def along_y(move, values):
    moved = []
    for n, value in enumerate(values, 1):
        moved.append(move(value, n))
    return moved


def three_parts(total):
    high = total.astype(bf16)
    rest = total - high.astype(f32)
    middle = rest.astype(bf16)
    low = (rest - middle.astype(f32)).astype(bf16)
    return high, middle, low


def live_kernel(size_ref, wave_ref, live_ref, copies_ref):
    rows, width = wave_ref.shape
    size = size_ref[0]
    row = lax.axis_index(OP) * rows + lax.broadcasted_iota(jnp.int32, (rows, width), 0)
    col = lax.broadcasted_iota(jnp.int32, (rows, width), 1)
    wave = wave_ref[...].astype(f32)
    live = jnp.where((row < size) & (col < size), wave, 0.0).astype(bf16)
    live_ref[...] = live
    for z in range(copies_ref.shape[0]):
        copies_ref[z] = live


def choose_kernel(steps, partner_ref, live_ref, *refs):
    got_refs, copies_ref = refs[:-1], refs[-1]
    partner = partner_ref[lax.axis_index(SEC)]

    def place(ref):
        value = ref[...]
        for z in range(copies_ref.shape[0]):
            copies_ref[z] = value

    @pl.when(partner == lax.axis_index(SEC))
    def _():
        place(live_ref)

    for step, ref in zip(steps, got_refs):

        @pl.when(partner == sector_behind(step))
        def _(ref=ref):
            place(ref)


def products(x_refs, operators, outs, scratch, first_dims, second_dims):
    left_hbm, right_hbm = operators
    x_all, half, left_ref, right_ref, arrived = scratch
    count = len(x_refs)
    ahead = lax.axis_index(Y)
    rows = x_refs[0].shape[0]
    terms, width, _ = left_ref.shape
    copies = []
    for k in range(terms):
        copies.append((left_hbm, left_ref, 0, k))
        if k:
            copies.append((right_hbm, right_ref, 1, k - 1))
    copies.append((right_hbm, right_ref, 1, terms - 1))
    copies = [
        pltpu.make_async_copy(hbm.at[k], ref.at[k], arrived.at[side, k])
        for hbm, ref, side, k in copies
    ]
    copies[0].start()
    copies[1].start()
    for step, ref in enumerate(x_refs):
        place = pl.multiple_of(lax.rem(ahead + step, count) * rows, rows)
        x_all[pl.ds(place, rows), :] = ref[...]
    total = None
    for n in range(2 * terms):
        copies[n].wait()
        if n + 2 < 2 * terms:
            copies[n + 2].start()
        if n == 0 or (n % 2 and n < 2 * terms - 1):
            k = (n + 1) // 2
            first = lax.dot_general(
                left_ref[k], x_all[...], first_dims, preferred_element_type=f32
            ).astype(bf16)
            for block in range(count):
                place = pl.multiple_of(lax.rem(block - ahead + count, count) * rows, rows)
                half[pl.ds(place, rows), k * width : (k + 1) * width] = first[
                    block * rows : (block + 1) * rows
                ]
        else:
            k = n // 2 - 1 if n < 2 * terms - 1 else terms - 1
            part = lax.dot_general(
                half[:, k * width : (k + 1) * width],
                right_ref[k],
                second_dims,
                preferred_element_type=f32,
            )
            total = part if total is None else total + part
    for step in range(count):
        outs[step][...] = total[step * rows : (step + 1) * rows].astype(outs[step].dtype)


def adjoint_kernel(count, left_hbm, right_hbm, *refs):
    products(
        refs[:count], (left_hbm, right_hbm), refs[count : 2 * count], refs[2 * count :], TN, NN
    )


def direct_kernel(count, left_hbm, right_hbm, *refs):
    products(
        refs[:count], (left_hbm, right_hbm), refs[count : 2 * count], refs[2 * count :], NN, NT
    )


def sums_kernel(count, live_ref, diagonal_ref, *refs):
    x_refs, adjoint_refs, outs = refs[:count], refs[count : 2 * count], refs[2 * count :]
    wave = live_ref[...].astype(f32)
    square = wave * wave
    norm = jnp.sum(square, axis=0, keepdims=True)
    mixed = jnp.sum(square * diagonal_ref[...], axis=0, keepdims=True)
    for x_ref, adjoint_ref in zip(x_refs, adjoint_refs):
        pair = x_ref[...].astype(f32) * adjoint_ref[...].astype(f32)
        mixed += 2.0 * jnp.sum(pair, axis=0, keepdims=True)
    mixed = jnp.sum(mixed, axis=1, keepdims=True)
    norm = jnp.sum(norm, axis=1, keepdims=True)
    sums_ref, sent_refs = outs[0], outs[1:]
    tile = sums_ref.shape
    row = lax.broadcasted_iota(jnp.int32, tile, 0)
    sums_ref[...] = jnp.where(
        row == 0, jnp.broadcast_to(mixed, tile), jnp.broadcast_to(norm, tile)
    )
    rows, width = adjoint_refs[1].shape
    tail = (sent_refs[0].shape[0] - rows, width)
    row = lax.broadcasted_iota(jnp.int32, tail, 0)
    extra = jnp.zeros(tail, f32)
    for place, part in enumerate(three_parts(mixed) + three_parts(norm)):
        extra = jnp.where(row == place, jnp.broadcast_to(part.astype(f32), tail), extra)
    extra = extra.astype(bf16)
    for adjoint_ref, sent_ref in zip(adjoint_refs[1:], sent_refs):
        sent_ref[:rows, :] = adjoint_ref[...]
        sent_ref[rows:, :] = extra


def tiles_of(rows, width):
    return [(r, c) for r in range(0, rows, 8) for c in range(0, width, 128)]


def rows_kernel(count, *refs):
    blocks, sums_refs, out_ref = refs[:count], refs[count:-1], refs[-1]
    rows, width = blocks[0].shape
    peers = out_ref.shape[0]
    each = rows // peers
    for pair in range(0, peers, 2):
        part = slice(pair * each, (pair + 2) * each)
        total = blocks[0][part, :].astype(f32)
        for ref in blocks[1:]:
            total += ref[part, :].astype(f32)
        for z in range(2):
            for n, (r, c) in enumerate(tiles_of(each, width)):
                out_ref[pair + z, 8 * n : 8 * n + 8, :] = total[
                    z * each + r : z * each + r + 8, c : c + 128
                ]
    if sums_refs:
        tile = sums_refs[0][...]
        mixed, norm = tile[0:1, :], tile[1:2, :]
        for ref in blocks[1:]:
            extra = ref[rows:, 0:128].astype(f32)
            mixed += extra[0:1] + extra[1:2] + extra[2:3]
            norm += extra[3:4] + extra[4:5] + extra[5:6]
        row = lax.broadcasted_iota(jnp.int32, tile.shape, 0)
        whole = jnp.where(row == 0, mixed, norm)
        for z in range(peers):
            out_ref[z, out_ref.shape[1] - 8 :, :] = whole


def meet_kernel(got_ref, out_ref):
    total = got_ref[0]
    for z in range(1, got_ref.shape[0]):
        total += got_ref[z]
    out_ref[...] = total


def update_kernel(
    steps, partner_ref, size_ref, direct_ref, diagonal_ref, live_ref, *refs
):
    got_refs, (updated_ref, residual_ref, routed) = refs[:-3], refs[-3:]
    rows, width = live_ref.shape
    peers, length, _ = direct_ref.shape
    me = lax.axis_index(SEC)
    sums = None
    for step, got_ref in zip([(0, 0)] + steps, got_refs):
        part = got_ref[length:, :]
        sums = part if sums is None else sums + part

        @pl.when(partner_ref[sector_behind(step)] == me)
        def _(got_ref=got_ref):
            routed[...] = got_ref[:length, :]

    energy = sums[0:1, :] / sums[1:2, :]
    size = size_ref[0]
    base = lax.axis_index(OP) * rows
    for n, (r, c) in enumerate(tiles_of(rows, width)):
        where_row = base + r + lax.broadcasted_iota(jnp.int32, (8, 128), 0)
        where_col = c + lax.broadcasted_iota(jnp.int32, (8, 128), 1)
        wave = live_ref[r : r + 8, c : c + 128].astype(f32)
        diagonal = diagonal_ref[r : r + 8, c : c + 128]
        part = slice(8 * n, 8 * n + 8)
        direct = direct_ref[0, part, :]
        for z in range(1, peers):
            direct += direct_ref[z, part, :]
        sigma = direct + routed[part, :] + diagonal * wave
        sigma = jnp.where((where_row < size) & (where_col < size), sigma, 0.0)
        residual = sigma - energy * wave
        residual_ref[r : r + 8, c : c + 128] = residual
        updated_ref[r : r + 8, c : c + 128] = wave - residual / jnp.maximum(
            jnp.abs(diagonal - energy), 1.0
        )


def run(kernel, outs, specs, scratch=(), flops=0, bytes_accessed=2**20, limit=16):
    return pl.pallas_call(
        kernel,
        out_shape=outs,
        in_specs=specs,
        out_specs=jax.tree.map(lambda _: VMEM, outs),
        scratch_shapes=list(scratch),
        compiler_params=pltpu.CompilerParams(vmem_limit_bytes=limit * 2**20),
        cost_estimate=pl.CostEstimate(
            flops=flops, bytes_accessed=bytes_accessed, transcendentals=0
        ),
    )


def per_device(wavefunction, left_ops, right_ops, diagonal, sector_sizes, partner):
    _, rows, width = wavefunction.shape
    terms = left_ops.shape[1]
    lines, peers = lax.axis_size(Y), lax.axis_size(Z)
    left, right, diag = left_ops[0], right_ops[0], diagonal[0]
    block = peers * rows
    length = rows * width // 128
    steps = other_sectors()

    def shape(*dims, dtype=f32):
        return jax.ShapeDtypeStruct(dims, dtype)

    live, copies = run(
        live_kernel,
        [shape(rows, width, dtype=bf16), shape(peers, rows, width, dtype=bf16)],
        [SMEM, VMEM],
    )(sector_sizes, wavefunction[0])
    own = lax.all_to_all(copies, Z, 0, 0, tiled=True).reshape(block, width)
    others = []
    for step in steps:
        others.append(from_sector(live, step))
    copies = run(
        functools.partial(choose_kernel, steps),
        shape(peers, rows, width, dtype=bf16),
        [SMEM] + [VMEM] * (1 + len(steps)),
    )(partner, live, *others)
    theirs = lax.all_to_all(copies, Z, 0, 0, tiled=True).reshape(block, width)
    own_parts = [own] + along_y(from_ahead, [own] * (lines - 1))
    their_parts = [theirs] + along_y(from_ahead, [theirs] * (lines - 1))

    flops = 4 * terms * width**3
    scratch = [
        pltpu.VMEM((width, width), bf16),
        pltpu.VMEM((width, terms * width), bf16),
        pltpu.VMEM((terms, width, width), bf16),
        pltpu.VMEM((terms, width, width), bf16),
        pltpu.SemaphoreType.DMA((2, terms)),
    ]
    outs = [shape(block, width)] + [shape(block, width, dtype=bf16)] * (lines - 1)
    specs = [HBM, HBM] + [VMEM] * lines
    adjoint = run(
        functools.partial(adjoint_kernel, lines), outs, specs, scratch, flops, limit=50
    )(left, right, *own_parts)
    longer = shape(block + 16, width, dtype=bf16)
    sums, *sent = run(
        functools.partial(sums_kernel, lines),
        [shape(8, 128)] + [longer] * (lines - 1),
        [VMEM] * (2 + 2 * lines),
    )(live, diag, *their_parts, *adjoint)
    adjoint_got = along_y(to_ahead, sent)
    direct = run(
        functools.partial(direct_kernel, lines), outs, specs, scratch, flops, limit=50
    )(left, right, *their_parts)
    direct_got = along_y(to_ahead, direct[1:])

    adjoint_lines = run(
        functools.partial(rows_kernel, lines), shape(peers, length + 8, 128), [VMEM] * (lines + 1)
    )(adjoint[0], *adjoint_got, sums)
    adjoint_lines = lax.all_to_all(adjoint_lines, Z, 0, 0, tiled=True)
    adjoint_mine = run(meet_kernel, shape(length + 8, 128), [VMEM])(adjoint_lines)
    routed = [adjoint_mine] + [from_sector(adjoint_mine, step) for step in steps]
    direct_lines = run(
        functools.partial(rows_kernel, lines), shape(peers, length, 128), [VMEM] * lines
    )(direct[0], *direct_got)
    direct_mine = lax.all_to_all(direct_lines, Z, 0, 0, tiled=True)
    updated, residual = run(
        functools.partial(update_kernel, steps),
        [shape(rows, width)] * 2,
        [SMEM, SMEM] + [VMEM] * (3 + len(routed)),
        [pltpu.VMEM((length, 128), f32)],
    )(partner, sector_sizes, direct_mine, diag, live, *routed)
    return updated[None], residual[None]


def solution(mesh):
    finer = Mesh(mesh.devices.reshape(4, 2, 4, 8), SEC + OP)
    return jax.shard_map(
        per_device,
        mesh=finer,
        in_specs=(
            P(SEC, OP, None),
            P(SEC, OP, None, None),
            P(SEC, OP, None, None),
            P(SEC, OP, None),
            P(SEC),
            P(),
        ),
        out_specs=(P(SEC, OP, None), P(SEC, OP, None)),
        check_vma=False,
    )
```

```python
import functools

import jax
import jax.numpy as jnp
from jax import lax
from jax.experimental import pallas as pl
from jax.experimental.pallas import tpu as pltpu
from jax.sharding import Mesh
from jax.sharding import PartitionSpec as P


SEC = ("sec_0", "sec_1")
OP = ("op_0", "op_1")
Y, Z = OP
bf16 = jnp.bfloat16
f32 = jnp.float32
VMEM = pl.BlockSpec(memory_space=pltpu.VMEM)
SMEM = pl.BlockSpec(memory_space=pltpu.SMEM)
HBM = pl.BlockSpec(memory_space=pltpu.HBM)
NN = (((1,), (0,)), ((), ()))
TN = (((0,), (0,)), ((), ()))
NT = (((1,), (1,)), ((), ()))


def other_sectors():
    far, near = (lax.axis_size(name) for name in SEC)
    return [(i, j) for i in range(far) for j in range(near) if i or j]


def from_sector(value, step):
    far, near = (lax.axis_size(name) for name in SEC)
    pairs = [
        (i * near + j, (i + step[0]) % far * near + (j + step[1]) % near)
        for i in range(far)
        for j in range(near)
    ]
    return lax.ppermute(value, SEC, pairs)


def sector_behind(step):
    far, near = (lax.axis_size(name) for name in SEC)
    i = lax.rem(lax.axis_index(SEC[0]) - step[0] + far, far)
    j = lax.rem(lax.axis_index(SEC[1]) - step[1] + near, near)
    return i * near + j


def from_ahead(value, steps):
    peers = lax.axis_size(Y)
    return lax.ppermute(value, Y, [(i, (i - steps) % peers) for i in range(peers)])


def to_ahead(value, steps):
    peers = lax.axis_size(Y)
    return lax.ppermute(value, Y, [(i, (i + steps) % peers) for i in range(peers)])


def along_y(move, values):
    moved = []
    for n, value in enumerate(values, 1):
        moved.append(move(value, n))
    return moved


def live_kernel(steps, size_ref, partner_ref, wave_ref, live_ref, copies_ref, chosen_ref):
    rows, width = wave_ref.shape
    size = size_ref[0]
    row = lax.axis_index(OP) * rows + lax.broadcasted_iota(jnp.int32, (rows, width), 0)
    col = lax.broadcasted_iota(jnp.int32, (rows, width), 1)
    wave = wave_ref[...].astype(f32)
    live = jnp.where((row < size) & (col < size), wave, 0.0).astype(bf16)
    live_ref[...] = live
    for z in range(copies_ref.shape[0]):
        copies_ref[z] = live
    me = lax.axis_index(SEC)
    partner = partner_ref[me]
    row = lax.broadcasted_iota(jnp.int32, chosen_ref.shape, 0)
    chosen = jnp.zeros(chosen_ref.shape, f32)
    for n, step in enumerate(steps):
        sender = sector_behind(step)
        gives = jnp.where(sender == partner, 1.0, 0.0)
        takes = jnp.where(partner_ref[sender] == me, 1.0, 0.0)
        chosen = jnp.where(row == n, gives, chosen)
        chosen = jnp.where(row == len(steps) + n, takes, chosen)
    chosen_ref[...] = chosen


def choose_kernel(chosen_ref, *refs):
    got_refs, copies_ref = refs[:-1], refs[-1]
    chosen = chosen_ref[...]
    value = None
    for n, ref in enumerate(got_refs):
        part = ref[...].astype(f32)
        mark = jnp.broadcast_to(chosen[n : n + 1, 0:1], part.shape)
        value = part if value is None else jnp.where(mark > 0.0, part, value)
    value = value.astype(bf16)
    for z in range(copies_ref.shape[0]):
        copies_ref[z] = value


def load_kernel(left_hbm, right_hbm, left_ref, right_ref, arrived):
    copies = [
        pltpu.make_async_copy(left_hbm, left_ref, arrived.at[0]),
        pltpu.make_async_copy(right_hbm, right_ref, arrived.at[1]),
    ]
    for copy in copies:
        copy.start()
    for copy in copies:
        copy.wait()


def products(x_refs, operators, outs, scratch, first_dims, second_dims):
    left_ref, right_ref = operators
    x_all, half = scratch
    count = len(x_refs)
    ahead = lax.axis_index(Y)
    rows = x_refs[0].shape[0]
    terms, width, _ = left_ref.shape
    for step, ref in enumerate(x_refs):
        place = pl.multiple_of(lax.rem(ahead + step, count) * rows, rows)
        x_all[pl.ds(place, rows), :] = ref[...]
    for k in range(terms):
        first = lax.dot_general(
            left_ref[k], x_all[...], first_dims, preferred_element_type=f32
        ).astype(bf16)
        for block in range(count):
            place = pl.multiple_of(lax.rem(block - ahead + count, count) * rows, rows)
            half[pl.ds(place, rows), k * width : (k + 1) * width] = first[
                block * rows : (block + 1) * rows
            ]
    if second_dims == NN:
        right = right_ref[...].reshape(terms * width, width)
        total = lax.dot_general(half[...], right, NN, preferred_element_type=f32)
    else:
        total = None
        for k in range(terms):
            part = lax.dot_general(
                half[:, k * width : (k + 1) * width],
                right_ref[k],
                second_dims,
                preferred_element_type=f32,
            )
            total = part if total is None else total + part
    for step in range(count):
        outs[step][...] = total[step * rows : (step + 1) * rows].astype(outs[step].dtype)


def adjoint_kernel(count, left_ref, right_ref, *refs):
    products(
        refs[:count], (left_ref, right_ref), refs[count : 2 * count], refs[2 * count :], TN, NN
    )


def direct_kernel(count, left_ref, right_ref, *refs):
    products(
        refs[:count], (left_ref, right_ref), refs[count : 2 * count], refs[2 * count :], NN, NT
    )


def sums_kernel(count, live_ref, diagonal_ref, *refs):
    x_refs, adjoint_refs, sums_ref = refs[:count], refs[count : 2 * count], refs[2 * count]
    wave = live_ref[...].astype(f32)
    square = wave * wave
    norm = jnp.sum(square, axis=0, keepdims=True)
    mixed = jnp.sum(square * diagonal_ref[...], axis=0, keepdims=True)
    for x_ref, adjoint_ref in zip(x_refs, adjoint_refs):
        pair = x_ref[...].astype(f32) * adjoint_ref[...].astype(f32)
        mixed += 2.0 * jnp.sum(pair, axis=0, keepdims=True)
    mixed = jnp.sum(mixed, axis=1, keepdims=True)
    norm = jnp.sum(norm, axis=1, keepdims=True)
    tile = sums_ref.shape
    row = lax.broadcasted_iota(jnp.int32, tile, 0)
    sums_ref[...] = jnp.where(
        row == 0, jnp.broadcast_to(mixed, tile), jnp.broadcast_to(norm, tile)
    )


def tiles_of(rows, width):
    return [(r, c) for r in range(0, rows, 8) for c in range(0, width, 128)]


def rows_kernel(count, *refs):
    blocks, sums_refs, out_ref = refs[:count], refs[count:-1], refs[-1]
    rows, width = blocks[0].shape
    peers = out_ref.shape[0]
    each = rows // peers
    for pair in range(0, peers, 2):
        part = slice(pair * each, (pair + 2) * each)
        total = blocks[0][part, :].astype(f32)
        for ref in blocks[1:]:
            total += ref[part, :].astype(f32)
        for z in range(2):
            for n, (r, c) in enumerate(tiles_of(each, width)):
                out_ref[pair + z, 8 * n : 8 * n + 8, :] = total[
                    z * each + r : z * each + r + 8, c : c + 128
                ]
    if sums_refs:
        total = sums_refs[0][...]
        for ref in sums_refs[1:]:
            total += ref[...]
        for z in range(peers):
            out_ref[z, out_ref.shape[1] - 8 :, :] = total


def meet_kernel(got_ref, out_ref):
    total = got_ref[0]
    for z in range(1, got_ref.shape[0]):
        total += got_ref[z]
    out_ref[...] = total


def update_kernel(size_ref, chosen_ref, direct_ref, diagonal_ref, live_ref, *refs):
    got_refs, (updated_ref, residual_ref, routed) = refs[:-3], refs[-3:]
    rows, width = live_ref.shape
    peers, length, _ = direct_ref.shape
    chosen = chosen_ref[...]
    value = sums = None
    for n, got_ref in enumerate(got_refs):
        part = got_ref[:length, :]
        mark = jnp.broadcast_to(chosen[len(got_refs) + n : len(got_refs) + n + 1, :], part.shape)
        value = part if value is None else jnp.where(mark > 0.0, part, value)
        tile = got_ref[length:, :]
        sums = tile if sums is None else sums + tile
    routed[...] = value
    energy = sums[0:1, :] / sums[1:2, :]
    size = size_ref[0]
    base = lax.axis_index(OP) * rows
    for n, (r, c) in enumerate(tiles_of(rows, width)):
        where_row = base + r + lax.broadcasted_iota(jnp.int32, (8, 128), 0)
        where_col = c + lax.broadcasted_iota(jnp.int32, (8, 128), 1)
        wave = live_ref[r : r + 8, c : c + 128].astype(f32)
        diagonal = diagonal_ref[r : r + 8, c : c + 128]
        part = slice(8 * n, 8 * n + 8)
        direct = direct_ref[0, part, :]
        for z in range(1, peers):
            direct += direct_ref[z, part, :]
        sigma = direct + routed[part, :] + diagonal * wave
        sigma = jnp.where((where_row < size) & (where_col < size), sigma, 0.0)
        residual = sigma - energy * wave
        residual_ref[r : r + 8, c : c + 128] = residual
        updated_ref[r : r + 8, c : c + 128] = wave - residual / jnp.maximum(
            jnp.abs(diagonal - energy), 1.0
        )


def run(kernel, outs, specs, scratch=(), flops=0, bytes_accessed=2**20, limit=16):
    return pl.pallas_call(
        kernel,
        out_shape=outs,
        in_specs=specs,
        out_specs=jax.tree.map(lambda _: VMEM, outs),
        scratch_shapes=list(scratch),
        compiler_params=pltpu.CompilerParams(vmem_limit_bytes=limit * 2**20),
        cost_estimate=pl.CostEstimate(
            flops=flops, bytes_accessed=bytes_accessed, transcendentals=0
        ),
    )


def per_device(wavefunction, left_ops, right_ops, diagonal, sector_sizes, partner):
    _, rows, width = wavefunction.shape
    terms = left_ops.shape[1]
    lines, peers = lax.axis_size(Y), lax.axis_size(Z)
    left, right, diag = left_ops[0], right_ops[0], diagonal[0]
    block = peers * rows
    length = rows * width // 128
    steps = other_sectors()

    def shape(*dims, dtype=f32):
        return jax.ShapeDtypeStruct(dims, dtype)

    every = [(0, 0)] + steps
    live, copies, chosen = run(
        functools.partial(live_kernel, every),
        [
            shape(rows, width, dtype=bf16),
            shape(peers, rows, width, dtype=bf16),
            shape(2 * len(every), 128),
        ],
        [SMEM, SMEM, VMEM],
    )(sector_sizes, partner, wavefunction[0])
    own = lax.all_to_all(copies, Z, 0, 0, tiled=True).reshape(block, width)
    others = []
    for step in steps:
        others.append(from_sector(live, step))
    copies = run(
        choose_kernel, shape(peers, rows, width, dtype=bf16), [VMEM] * (1 + len(every))
    )(chosen, live, *others)
    theirs = lax.all_to_all(copies, Z, 0, 0, tiled=True).reshape(block, width)
    own_parts = [own] + along_y(from_ahead, [own] * (lines - 1))
    their_parts = [theirs] + along_y(from_ahead, [theirs] * (lines - 1))

    flops = 4 * terms * width**3
    scratch = [pltpu.VMEM((width, width), bf16), pltpu.VMEM((width, terms * width), bf16)]

    def loaded():
        return run(
            load_kernel,
            [shape(*left.shape, dtype=bf16), shape(*right.shape, dtype=bf16)],
            [HBM, HBM],
            [pltpu.SemaphoreType.DMA((2,))],
            bytes_accessed=2 * (left.size + right.size),
            limit=46,
        )(left, right)

    outs = [shape(block, width)] + [shape(block, width, dtype=bf16)] * (lines - 1)
    specs = [VMEM] * (2 + lines)
    adjoint = run(
        functools.partial(adjoint_kernel, lines), outs, specs, scratch, flops, limit=44
    )(*loaded(), *own_parts)
    adjoint_got = along_y(to_ahead, adjoint[1:])
    sums = run(
        functools.partial(sums_kernel, lines), shape(8, 128), [VMEM] * (2 + 2 * lines)
    )(live, diag, *their_parts, *adjoint)
    sums_got = along_y(to_ahead, [sums] * (lines - 1))
    direct = run(
        functools.partial(direct_kernel, lines), outs, specs, scratch, flops, limit=44
    )(*loaded(), *their_parts)
    direct_got = along_y(to_ahead, direct[1:])

    adjoint_lines = run(
        functools.partial(rows_kernel, lines), shape(peers, length + 8, 128), [VMEM] * (2 * lines)
    )(adjoint[0], *adjoint_got, sums, *sums_got)
    adjoint_lines = lax.all_to_all(adjoint_lines, Z, 0, 0, tiled=True)
    adjoint_mine = run(meet_kernel, shape(length + 8, 128), [VMEM])(adjoint_lines)
    routed = [adjoint_mine] + [from_sector(adjoint_mine, step) for step in steps]
    direct_lines = run(
        functools.partial(rows_kernel, lines), shape(peers, length, 128), [VMEM] * lines
    )(direct[0], *direct_got)
    direct_mine = lax.all_to_all(direct_lines, Z, 0, 0, tiled=True)
    updated, residual = run(
        update_kernel,
        [shape(rows, width)] * 2,
        [SMEM] + [VMEM] * (4 + len(routed)),
        [pltpu.VMEM((length, 128), f32)],
    )(sector_sizes, chosen, direct_mine, diag, live, *routed)
    return updated[None], residual[None]


def solution(mesh):
    finer = Mesh(mesh.devices.reshape(4, 2, 4, 8), SEC + OP)
    return jax.shard_map(
        per_device,
        mesh=finer,
        in_specs=(
            P(SEC, OP, None),
            P(SEC, OP, None, None),
            P(SEC, OP, None, None),
            P(SEC, OP, None),
            P(SEC),
            P(),
        ),
        out_specs=(P(SEC, OP, None), P(SEC, OP, None)),
        check_vma=False,
    )
```

```python
import functools

import jax
import jax.numpy as jnp
from jax import lax
from jax.experimental import pallas as pl
from jax.experimental.pallas import tpu as pltpu
from jax.sharding import Mesh
from jax.sharding import PartitionSpec as P


SEC = ("sec_0", "sec_1")
OP = ("op_0", "op_1")
Y, Z = OP
bf16 = jnp.bfloat16
f32 = jnp.float32
VMEM = pl.BlockSpec(memory_space=pltpu.VMEM)
SMEM = pl.BlockSpec(memory_space=pltpu.SMEM)
HBM = pl.BlockSpec(memory_space=pltpu.HBM)
NN = (((1,), (0,)), ((), ()))
TN = (((0,), (0,)), ((), ()))
NT = (((1,), (1,)), ((), ()))


def other_sectors():
    far, near = (lax.axis_size(name) for name in SEC)
    return [(i, j) for i in range(far) for j in range(near) if i or j]


def from_sector(value, step):
    far, near = (lax.axis_size(name) for name in SEC)
    pairs = [
        (i * near + j, (i + step[0]) % far * near + (j + step[1]) % near)
        for i in range(far)
        for j in range(near)
    ]
    return lax.ppermute(value, SEC, pairs)


def sector_behind(step):
    far, near = (lax.axis_size(name) for name in SEC)
    i = lax.rem(lax.axis_index(SEC[0]) - step[0] + far, far)
    j = lax.rem(lax.axis_index(SEC[1]) - step[1] + near, near)
    return i * near + j


def from_ahead(value, steps):
    peers = lax.axis_size(Y)
    return lax.ppermute(value, Y, [(i, (i - steps) % peers) for i in range(peers)])


def to_ahead(value, steps):
    peers = lax.axis_size(Y)
    return lax.ppermute(value, Y, [(i, (i + steps) % peers) for i in range(peers)])


def along_y(move, values):
    moved = []
    for n, value in enumerate(values, 1):
        moved.append(move(value, n))
    return moved


def live_kernel(size_ref, wave_ref, live_ref, copies_ref):
    rows, width = wave_ref.shape
    size = size_ref[0]
    row = lax.axis_index(OP) * rows + lax.broadcasted_iota(jnp.int32, (rows, width), 0)
    col = lax.broadcasted_iota(jnp.int32, (rows, width), 1)
    wave = wave_ref[...].astype(f32)
    live = jnp.where((row < size) & (col < size), wave, 0.0).astype(bf16)
    live_ref[...] = live
    for z in range(copies_ref.shape[0]):
        copies_ref[z] = live


def chosen_kernel(steps, partner_ref, chosen_ref):
    me = lax.axis_index(SEC)
    partner = partner_ref[me]
    row = lax.broadcasted_iota(jnp.int32, chosen_ref.shape, 0)
    chosen = jnp.zeros(chosen_ref.shape, f32)
    for n, step in enumerate(steps):
        sender = sector_behind(step)
        gives = jnp.where(sender == partner, 1.0, 0.0)
        takes = jnp.where(partner_ref[sender] == me, 1.0, 0.0)
        chosen = jnp.where(row == n, gives, chosen)
        chosen = jnp.where(row == len(steps) + n, takes, chosen)
    chosen_ref[...] = chosen


def choose_kernel(chosen_ref, *refs):
    got_refs, copies_ref = refs[:-1], refs[-1]
    chosen = chosen_ref[...]
    value = None
    for n, ref in enumerate(got_refs):
        part = ref[...].astype(f32)
        mark = jnp.broadcast_to(chosen[n : n + 1, 0:1], part.shape)
        value = part if value is None else jnp.where(mark > 0.0, part, value)
    value = value.astype(bf16)
    for z in range(copies_ref.shape[0]):
        copies_ref[z] = value


def load_kernel(left_hbm, right_hbm, left_ref, right_ref, arrived):
    copies = [
        pltpu.make_async_copy(left_hbm, left_ref, arrived.at[0]),
        pltpu.make_async_copy(right_hbm, right_ref, arrived.at[1]),
    ]
    for copy in copies:
        copy.start()
    for copy in copies:
        copy.wait()


def products(x_refs, operators, outs, scratch, first_dims, second_dims):
    left_ref, right_ref = operators
    x_all, half = scratch
    count = len(x_refs)
    ahead = lax.axis_index(Y)
    rows = x_refs[0].shape[0]
    terms, width, _ = left_ref.shape
    for step, ref in enumerate(x_refs):
        place = pl.multiple_of(lax.rem(ahead + step, count) * rows, rows)
        x_all[pl.ds(place, rows), :] = ref[...]
    for k in range(terms):
        first = lax.dot_general(
            left_ref[k], x_all[...], first_dims, preferred_element_type=f32
        ).astype(bf16)
        for block in range(count):
            place = pl.multiple_of(lax.rem(block - ahead + count, count) * rows, rows)
            half[pl.ds(place, rows), k * width : (k + 1) * width] = first[
                block * rows : (block + 1) * rows
            ]
    if second_dims == NN:
        right = right_ref[...].reshape(terms * width, width)
        total = lax.dot_general(half[...], right, NN, preferred_element_type=f32)
    else:
        total = None
        for k in range(terms):
            part = lax.dot_general(
                half[:, k * width : (k + 1) * width],
                right_ref[k],
                second_dims,
                preferred_element_type=f32,
            )
            total = part if total is None else total + part
    for step in range(count):
        outs[step][...] = total[step * rows : (step + 1) * rows].astype(outs[step].dtype)


def adjoint_kernel(count, left_ref, right_ref, *refs):
    products(
        refs[:count], (left_ref, right_ref), refs[count : 2 * count], refs[2 * count :], TN, NN
    )


def direct_kernel(count, left_ref, right_ref, *refs):
    products(
        refs[:count], (left_ref, right_ref), refs[count : 2 * count], refs[2 * count :], NN, NT
    )


def sums_kernel(count, live_ref, diagonal_ref, *refs):
    x_refs, adjoint_refs, sums_ref = refs[:count], refs[count : 2 * count], refs[2 * count]
    wave = live_ref[...].astype(f32)
    square = wave * wave
    norm = jnp.sum(square, axis=0, keepdims=True)
    mixed = jnp.sum(square * diagonal_ref[...], axis=0, keepdims=True)
    for x_ref, adjoint_ref in zip(x_refs, adjoint_refs):
        pair = x_ref[...].astype(f32) * adjoint_ref[...].astype(f32)
        mixed += 2.0 * jnp.sum(pair, axis=0, keepdims=True)
    mixed = jnp.sum(mixed, axis=1, keepdims=True)
    norm = jnp.sum(norm, axis=1, keepdims=True)
    tile = sums_ref.shape
    row = lax.broadcasted_iota(jnp.int32, tile, 0)
    sums_ref[...] = jnp.where(
        row == 0, jnp.broadcast_to(mixed, tile), jnp.broadcast_to(norm, tile)
    )


def tiles_of(rows, width):
    return [(r, c) for r in range(0, rows, 8) for c in range(0, width, 128)]


def rows_kernel(count, *refs):
    blocks, sums_refs, out_ref = refs[:count], refs[count:-1], refs[-1]
    rows, width = blocks[0].shape
    peers = out_ref.shape[0]
    each = rows // peers
    for pair in range(0, peers, 2):
        part = slice(pair * each, (pair + 2) * each)
        total = blocks[0][part, :].astype(f32)
        for ref in blocks[1:]:
            total += ref[part, :].astype(f32)
        for z in range(2):
            for n, (r, c) in enumerate(tiles_of(each, width)):
                out_ref[pair + z, 8 * n : 8 * n + 8, :] = total[
                    z * each + r : z * each + r + 8, c : c + 128
                ]
    if sums_refs:
        total = sums_refs[0][...]
        for ref in sums_refs[1:]:
            total += ref[...]
        for z in range(peers):
            out_ref[z, out_ref.shape[1] - 8 :, :] = total


def meet_kernel(got_ref, out_ref):
    total = got_ref[0]
    for z in range(1, got_ref.shape[0]):
        total += got_ref[z]
    out_ref[...] = total


def update_kernel(size_ref, chosen_ref, direct_ref, diagonal_ref, live_ref, *refs):
    got_refs, (updated_ref, residual_ref, routed) = refs[:-3], refs[-3:]
    rows, width = live_ref.shape
    peers, length, _ = direct_ref.shape
    chosen = chosen_ref[...]
    value = sums = None
    for n, got_ref in enumerate(got_refs):
        part = got_ref[:length, :]
        mark = jnp.broadcast_to(chosen[len(got_refs) + n : len(got_refs) + n + 1, :], part.shape)
        value = part if value is None else jnp.where(mark > 0.0, part, value)
        tile = got_ref[length:, :]
        sums = tile if sums is None else sums + tile
    routed[...] = value
    energy = sums[0:1, :] / sums[1:2, :]
    size = size_ref[0]
    base = lax.axis_index(OP) * rows
    for n, (r, c) in enumerate(tiles_of(rows, width)):
        where_row = base + r + lax.broadcasted_iota(jnp.int32, (8, 128), 0)
        where_col = c + lax.broadcasted_iota(jnp.int32, (8, 128), 1)
        wave = live_ref[r : r + 8, c : c + 128].astype(f32)
        diagonal = diagonal_ref[r : r + 8, c : c + 128]
        part = slice(8 * n, 8 * n + 8)
        direct = direct_ref[0, part, :]
        for z in range(1, peers):
            direct += direct_ref[z, part, :]
        sigma = direct + routed[part, :] + diagonal * wave
        sigma = jnp.where((where_row < size) & (where_col < size), sigma, 0.0)
        residual = sigma - energy * wave
        residual_ref[r : r + 8, c : c + 128] = residual
        updated_ref[r : r + 8, c : c + 128] = wave - residual / jnp.maximum(
            jnp.abs(diagonal - energy), 1.0
        )


def run(kernel, outs, specs, scratch=(), flops=0, bytes_accessed=2**20, limit=16):
    return pl.pallas_call(
        kernel,
        out_shape=outs,
        in_specs=specs,
        out_specs=jax.tree.map(lambda _: VMEM, outs),
        scratch_shapes=list(scratch),
        compiler_params=pltpu.CompilerParams(vmem_limit_bytes=limit * 2**20),
        cost_estimate=pl.CostEstimate(
            flops=flops, bytes_accessed=bytes_accessed, transcendentals=0
        ),
    )


def per_device(wavefunction, left_ops, right_ops, diagonal, sector_sizes, partner):
    _, rows, width = wavefunction.shape
    terms = left_ops.shape[1]
    lines, peers = lax.axis_size(Y), lax.axis_size(Z)
    left, right, diag = left_ops[0], right_ops[0], diagonal[0]
    block = peers * rows
    length = rows * width // 128
    steps = other_sectors()

    def shape(*dims, dtype=f32):
        return jax.ShapeDtypeStruct(dims, dtype)

    every = [(0, 0)] + steps
    live, copies = run(
        live_kernel,
        [shape(rows, width, dtype=bf16), shape(peers, rows, width, dtype=bf16)],
        [SMEM, VMEM],
    )(sector_sizes, wavefunction[0])
    chosen = run(
        functools.partial(chosen_kernel, every), shape(2 * len(every), 128), [SMEM]
    )(partner)
    own = lax.all_to_all(copies, Z, 0, 0, tiled=True).reshape(block, width)
    others = []
    for step in steps:
        others.append(from_sector(live, step))
    copies = run(
        choose_kernel, shape(peers, rows, width, dtype=bf16), [VMEM] * (1 + len(every))
    )(chosen, live, *others)
    theirs = lax.all_to_all(copies, Z, 0, 0, tiled=True).reshape(block, width)
    own_parts = [own] + along_y(from_ahead, [own] * (lines - 1))
    their_parts = [theirs] + along_y(from_ahead, [theirs] * (lines - 1))

    flops = 4 * terms * width**3
    scratch = [pltpu.VMEM((width, width), bf16), pltpu.VMEM((width, terms * width), bf16)]

    def loaded():
        return run(
            load_kernel,
            [shape(*left.shape, dtype=bf16), shape(*right.shape, dtype=bf16)],
            [HBM, HBM],
            [pltpu.SemaphoreType.DMA((2,))],
            bytes_accessed=2 * (left.size + right.size),
            limit=46,
        )(left, right)

    outs = [shape(block, width)] + [shape(block, width, dtype=bf16)] * (lines - 1)
    specs = [VMEM] * (2 + lines)
    adjoint = run(
        functools.partial(adjoint_kernel, lines), outs, specs, scratch, flops, limit=44
    )(*loaded(), *own_parts)
    adjoint_got = along_y(to_ahead, adjoint[1:])
    sums = run(
        functools.partial(sums_kernel, lines), shape(8, 128), [VMEM] * (2 + 2 * lines)
    )(live, diag, *their_parts, *adjoint)
    sums_got = along_y(to_ahead, [sums] * (lines - 1))
    direct = run(
        functools.partial(direct_kernel, lines), outs, specs, scratch, flops, limit=44
    )(*loaded(), *their_parts)
    direct_got = along_y(to_ahead, direct[1:])

    adjoint_lines = run(
        functools.partial(rows_kernel, lines), shape(peers, length + 8, 128), [VMEM] * (2 * lines)
    )(adjoint[0], *adjoint_got, sums, *sums_got)
    adjoint_lines = lax.all_to_all(adjoint_lines, Z, 0, 0, tiled=True)
    adjoint_mine = run(meet_kernel, shape(length + 8, 128), [VMEM])(adjoint_lines)
    routed = [adjoint_mine] + [from_sector(adjoint_mine, step) for step in steps]
    direct_lines = run(
        functools.partial(rows_kernel, lines), shape(peers, length, 128), [VMEM] * lines
    )(direct[0], *direct_got)
    direct_mine = lax.all_to_all(direct_lines, Z, 0, 0, tiled=True)
    updated, residual = run(
        update_kernel,
        [shape(rows, width)] * 2,
        [SMEM] + [VMEM] * (4 + len(routed)),
        [pltpu.VMEM((length, 128), f32)],
    )(sector_sizes, chosen, direct_mine, diag, live, *routed)
    return updated[None], residual[None]


def solution(mesh):
    finer = Mesh(mesh.devices.reshape(4, 2, 4, 8), SEC + OP)
    return jax.shard_map(
        per_device,
        mesh=finer,
        in_specs=(
            P(SEC, OP, None),
            P(SEC, OP, None, None),
            P(SEC, OP, None, None),
            P(SEC, OP, None),
            P(SEC),
            P(),
        ),
        out_specs=(P(SEC, OP, None), P(SEC, OP, None)),
        check_vma=False,
    )
```

```python
import functools

import jax
import jax.numpy as jnp
from jax import lax
from jax.experimental import pallas as pl
from jax.experimental.pallas import tpu as pltpu
from jax.sharding import Mesh
from jax.sharding import PartitionSpec as P


SEC = ("sec_0", "sec_1")
OP = ("op_0", "op_1")
Y, Z = OP
bf16 = jnp.bfloat16
f32 = jnp.float32
VMEM = pl.BlockSpec(memory_space=pltpu.VMEM)
SMEM = pl.BlockSpec(memory_space=pltpu.SMEM)
HBM = pl.BlockSpec(memory_space=pltpu.HBM)
NN = (((1,), (0,)), ((), ()))
TN = (((0,), (0,)), ((), ()))
NT = (((1,), (1,)), ((), ()))


def other_sectors():
    far, near = (lax.axis_size(name) for name in SEC)
    steps = [(i, j) for i in range(far) for j in range(near) if i or j]
    return sorted(steps, key=lambda step: (min(step[0], far - step[0]), step[1]))


def from_sector(value, step):
    far, near = (lax.axis_size(name) for name in SEC)
    pairs = [
        (i * near + j, (i + step[0]) % far * near + (j + step[1]) % near)
        for i in range(far)
        for j in range(near)
    ]
    return lax.ppermute(value, SEC, pairs)


def sector_behind(step):
    far, near = (lax.axis_size(name) for name in SEC)
    i = lax.rem(lax.axis_index(SEC[0]) - step[0] + far, far)
    j = lax.rem(lax.axis_index(SEC[1]) - step[1] + near, near)
    return i * near + j


def from_ahead(value, steps):
    peers = lax.axis_size(Y)
    return lax.ppermute(value, Y, [(i, (i - steps) % peers) for i in range(peers)])


def to_ahead(value, steps):
    peers = lax.axis_size(Y)
    return lax.ppermute(value, Y, [(i, (i + steps) % peers) for i in range(peers)])


def along_y(move, values):
    moved = []
    for n, value in enumerate(values, 1):
        moved.append(move(value, n))
    return moved


def live_kernel(size_ref, wave_ref, live_ref, copies_ref):
    rows, width = wave_ref.shape
    size = size_ref[0]
    row = lax.axis_index(OP) * rows + lax.broadcasted_iota(jnp.int32, (rows, width), 0)
    col = lax.broadcasted_iota(jnp.int32, (rows, width), 1)
    wave = wave_ref[...].astype(f32)
    live = jnp.where((row < size) & (col < size), wave, 0.0).astype(bf16)
    live_ref[...] = live
    for z in range(copies_ref.shape[0]):
        copies_ref[z] = live


def chosen_kernel(steps, partner_ref, chosen_ref):
    me = lax.axis_index(SEC)
    partner = partner_ref[me]
    row = lax.broadcasted_iota(jnp.int32, chosen_ref.shape, 0)
    chosen = jnp.zeros(chosen_ref.shape, f32)
    for n, step in enumerate(steps):
        sender = sector_behind(step)
        gives = jnp.where(sender == partner, 1.0, 0.0)
        takes = jnp.where(partner_ref[sender] == me, 1.0, 0.0)
        chosen = jnp.where(row == n, gives, chosen)
        chosen = jnp.where(row == len(steps) + n, takes, chosen)
    chosen_ref[...] = chosen


def choose_kernel(chosen_ref, *refs):
    got_refs, copies_ref = refs[:-1], refs[-1]
    chosen = chosen_ref[...]
    value = None
    for n, ref in enumerate(got_refs):
        part = ref[...].astype(f32)
        mark = jnp.broadcast_to(chosen[n : n + 1, 0:1], part.shape)
        value = part if value is None else jnp.where(mark > 0.0, part, value)
    value = value.astype(bf16)
    for z in range(copies_ref.shape[0]):
        copies_ref[z] = value


def load_kernel(left_hbm, right_hbm, left_ref, right_ref, arrived):
    copies = [
        pltpu.make_async_copy(left_hbm, left_ref, arrived.at[0]),
        pltpu.make_async_copy(right_hbm, right_ref, arrived.at[1]),
    ]
    for copy in copies:
        copy.start()
    for copy in copies:
        copy.wait()


def products(x_refs, operators, outs, scratch, first_dims, second_dims):
    left_ref, right_ref = operators
    x_all, half = scratch
    count = len(x_refs)
    ahead = lax.axis_index(Y)
    rows = x_refs[0].shape[0]
    terms, width, _ = left_ref.shape
    for step, ref in enumerate(x_refs):
        place = pl.multiple_of(lax.rem(ahead + step, count) * rows, rows)
        x_all[pl.ds(place, rows), :] = ref[...]
    for k in range(terms):
        first = lax.dot_general(
            left_ref[k], x_all[...], first_dims, preferred_element_type=f32
        ).astype(bf16)
        for block in range(count):
            place = pl.multiple_of(lax.rem(block - ahead + count, count) * rows, rows)
            half[pl.ds(place, rows), k * width : (k + 1) * width] = first[
                block * rows : (block + 1) * rows
            ]
    if second_dims == NN:
        right = right_ref[...].reshape(terms * width, width)
        total = lax.dot_general(half[...], right, NN, preferred_element_type=f32)
    else:
        total = None
        for k in range(terms):
            part = lax.dot_general(
                half[:, k * width : (k + 1) * width],
                right_ref[k],
                second_dims,
                preferred_element_type=f32,
            )
            total = part if total is None else total + part
    for step in range(count):
        outs[step][...] = total[step * rows : (step + 1) * rows].astype(outs[step].dtype)


def adjoint_kernel(count, left_ref, right_ref, *refs):
    products(
        refs[:count], (left_ref, right_ref), refs[count : 2 * count], refs[2 * count :], TN, NN
    )


def direct_kernel(count, left_ref, right_ref, *refs):
    products(
        refs[:count], (left_ref, right_ref), refs[count : 2 * count], refs[2 * count :], NN, NT
    )


def sums_kernel(count, live_ref, diagonal_ref, *refs):
    x_refs, adjoint_refs, sums_ref = refs[:count], refs[count : 2 * count], refs[2 * count]
    wave = live_ref[...].astype(f32)
    square = wave * wave
    norm = jnp.sum(square, axis=0, keepdims=True)
    mixed = jnp.sum(square * diagonal_ref[...], axis=0, keepdims=True)
    for x_ref, adjoint_ref in zip(x_refs, adjoint_refs):
        pair = x_ref[...].astype(f32) * adjoint_ref[...].astype(f32)
        mixed += 2.0 * jnp.sum(pair, axis=0, keepdims=True)
    mixed = jnp.sum(mixed, axis=1, keepdims=True)
    norm = jnp.sum(norm, axis=1, keepdims=True)
    tile = sums_ref.shape
    row = lax.broadcasted_iota(jnp.int32, tile, 0)
    sums_ref[...] = jnp.where(
        row == 0, jnp.broadcast_to(mixed, tile), jnp.broadcast_to(norm, tile)
    )


def tiles_of(rows, width):
    return [(r, c) for r in range(0, rows, 8) for c in range(0, width, 128)]


def rows_kernel(count, *refs):
    blocks, sums_refs, out_ref = refs[:count], refs[count:-1], refs[-1]
    rows, width = blocks[0].shape
    peers = out_ref.shape[0]
    each = rows // peers
    for pair in range(0, peers, 2):
        part = slice(pair * each, (pair + 2) * each)
        total = blocks[0][part, :].astype(f32)
        for ref in blocks[1:]:
            total += ref[part, :].astype(f32)
        for z in range(2):
            lines = total[z * each : (z + 1) * each]
            if not sums_refs:
                out_ref[pair + z] = lines.astype(out_ref.dtype)
                continue
            for n, (r, c) in enumerate(tiles_of(each, width)):
                out_ref[pair + z, 8 * n : 8 * n + 8, :] = lines[r : r + 8, c : c + 128]
    if sums_refs:
        total = sums_refs[0][...]
        for ref in sums_refs[1:]:
            total += ref[...]
        for z in range(peers):
            out_ref[z, out_ref.shape[1] - 8 :, :] = total


def meet_kernel(got_ref, out_ref):
    total = got_ref[0]
    for z in range(1, got_ref.shape[0]):
        total += got_ref[z]
    out_ref[...] = total


def update_kernel(size_ref, chosen_ref, direct_ref, diagonal_ref, live_ref, *refs):
    got_refs, (updated_ref, residual_ref, routed) = refs[:-3], refs[-3:]
    rows, width = live_ref.shape
    length = routed.shape[0]
    direct_all = direct_ref[0].astype(f32)
    for z in range(1, direct_ref.shape[0]):
        direct_all += direct_ref[z].astype(f32)
    chosen = chosen_ref[...]
    value = sums = None
    for n, got_ref in enumerate(got_refs):
        part = got_ref[:length, :]
        mark = jnp.broadcast_to(chosen[len(got_refs) + n : len(got_refs) + n + 1, :], part.shape)
        value = part if value is None else jnp.where(mark > 0.0, part, value)
        tile = got_ref[length:, :]
        sums = tile if sums is None else sums + tile
    routed[...] = value
    energy = sums[0:1, :] / sums[1:2, :]
    size = size_ref[0]
    base = lax.axis_index(OP) * rows
    for n, (r, c) in enumerate(tiles_of(rows, width)):
        where_row = base + r + lax.broadcasted_iota(jnp.int32, (8, 128), 0)
        where_col = c + lax.broadcasted_iota(jnp.int32, (8, 128), 1)
        wave = live_ref[r : r + 8, c : c + 128].astype(f32)
        diagonal = diagonal_ref[r : r + 8, c : c + 128]
        part = slice(8 * n, 8 * n + 8)
        direct = direct_all[r : r + 8, c : c + 128]
        sigma = direct + routed[part, :] + diagonal * wave
        sigma = jnp.where((where_row < size) & (where_col < size), sigma, 0.0)
        residual = sigma - energy * wave
        residual_ref[r : r + 8, c : c + 128] = residual
        updated_ref[r : r + 8, c : c + 128] = wave - residual / jnp.maximum(
            jnp.abs(diagonal - energy), 1.0
        )


def run(kernel, outs, specs, scratch=(), flops=0, bytes_accessed=2**20, limit=16):
    return pl.pallas_call(
        kernel,
        out_shape=outs,
        in_specs=specs,
        out_specs=jax.tree.map(lambda _: VMEM, outs),
        scratch_shapes=list(scratch),
        compiler_params=pltpu.CompilerParams(vmem_limit_bytes=limit * 2**20),
        cost_estimate=pl.CostEstimate(
            flops=flops, bytes_accessed=bytes_accessed, transcendentals=0
        ),
    )


def per_device(wavefunction, left_ops, right_ops, diagonal, sector_sizes, partner):
    _, rows, width = wavefunction.shape
    terms = left_ops.shape[1]
    lines, peers = lax.axis_size(Y), lax.axis_size(Z)
    left, right, diag = left_ops[0], right_ops[0], diagonal[0]
    block = peers * rows
    length = rows * width // 128
    steps = other_sectors()

    def shape(*dims, dtype=f32):
        return jax.ShapeDtypeStruct(dims, dtype)

    every = [(0, 0)] + steps
    live, copies = run(
        live_kernel,
        [shape(rows, width, dtype=bf16), shape(peers, rows, width, dtype=bf16)],
        [SMEM, VMEM],
    )(sector_sizes, wavefunction[0])
    chosen = run(
        functools.partial(chosen_kernel, every), shape(2 * len(every), 128), [SMEM]
    )(partner)
    own = lax.all_to_all(copies, Z, 0, 0, tiled=True).reshape(block, width)
    others = []
    for step in steps:
        others.append(from_sector(live, step))
    copies = run(
        choose_kernel, shape(peers, rows, width, dtype=bf16), [VMEM] * (1 + len(every))
    )(chosen, live, *others)
    theirs = lax.all_to_all(copies, Z, 0, 0, tiled=True).reshape(block, width)
    own_parts = [own] + along_y(from_ahead, [own] * (lines - 1))
    their_parts = [theirs] + along_y(from_ahead, [theirs] * (lines - 1))

    flops = 4 * terms * width**3
    scratch = [pltpu.VMEM((width, width), bf16), pltpu.VMEM((width, terms * width), bf16)]

    def loaded():
        return run(
            load_kernel,
            [shape(*left.shape, dtype=bf16), shape(*right.shape, dtype=bf16)],
            [HBM, HBM],
            [pltpu.SemaphoreType.DMA((2,))],
            bytes_accessed=2 * (left.size + right.size),
            limit=46,
        )(left, right)

    outs = [shape(block, width)] + [shape(block, width, dtype=bf16)] * (lines - 1)
    specs = [VMEM] * (2 + lines)
    adjoint = run(
        functools.partial(adjoint_kernel, lines), outs, specs, scratch, flops, limit=44
    )(*loaded(), *own_parts)
    adjoint_got = along_y(to_ahead, adjoint[1:])
    sums = run(
        functools.partial(sums_kernel, lines), shape(8, 128), [VMEM] * (2 + 2 * lines)
    )(live, diag, *their_parts, *adjoint)
    sums_got = along_y(to_ahead, [sums] * (lines - 1))
    direct = run(
        functools.partial(direct_kernel, lines), outs, specs, scratch, flops, limit=44
    )(*loaded(), *their_parts)
    direct_got = along_y(to_ahead, direct[1:])

    adjoint_lines = run(
        functools.partial(rows_kernel, lines), shape(peers, length + 8, 128), [VMEM] * (2 * lines)
    )(adjoint[0], *adjoint_got, sums, *sums_got)
    adjoint_lines = lax.all_to_all(adjoint_lines, Z, 0, 0, tiled=True)
    adjoint_mine = run(meet_kernel, shape(length + 8, 128), [VMEM])(adjoint_lines)
    routed = [adjoint_mine] + [from_sector(adjoint_mine, step) for step in steps]
    direct_lines = run(
        functools.partial(rows_kernel, lines), shape(peers, rows, width, dtype=bf16), [VMEM] * lines
    )(direct[0], *direct_got)
    direct_mine = lax.all_to_all(direct_lines, Z, 0, 0, tiled=True)
    updated, residual = run(
        update_kernel,
        [shape(rows, width)] * 2,
        [SMEM] + [VMEM] * (4 + len(routed)),
        [pltpu.VMEM((length, 128), f32)],
    )(sector_sizes, chosen, direct_mine, diag, live, *routed)
    return updated[None], residual[None]


def solution(mesh):
    finer = Mesh(mesh.devices.reshape(4, 2, 4, 8), SEC + OP)
    return jax.shard_map(
        per_device,
        mesh=finer,
        in_specs=(
            P(SEC, OP, None),
            P(SEC, OP, None, None),
            P(SEC, OP, None, None),
            P(SEC, OP, None),
            P(SEC),
            P(),
        ),
        out_specs=(P(SEC, OP, None), P(SEC, OP, None)),
        check_vma=False,
    )
```
